32 devices in a mesh: gp: 32 (over z, y, x, core).
Axes of the slice: x: 2, y: 2, z: 4, core: 2. Of those that a mesh axis runs over, the one named last changes fastest.
Arguments:
- grid_in: bfloat16 [16384, 474], P('gp')
- mesh_static: bfloat16 [16384, 3], P('gp')
- edge_static: bfloat16 [24576, 4], P('gp')
- send_rows: int32 [1024, 16], P('gp')
- edge_src: int32 [24576], P('gp')
- edge_dst: int32 [24576], P('gp')
- w_grid_in: bfloat16 [474, 512], replicated
- w_mesh_in: bfloat16 [3, 512], replicated
- w_edge_in: bfloat16 [4, 512], replicated
- w_edge_up: bfloat16 [1536, 512], replicated
- w_mesh_up: bfloat16 [1024, 512], replicated
- w_grid_up: bfloat16 [512, 512], replicated
- w_second: bfloat16 [6, 512, 512], replicated
- vectors: float32 [6, 4, 512], replicated
- d_mesh_out: bfloat16 [16384, 512], P('gp')
- d_grid_out: bfloat16 [16384, 512], P('gp')
Outputs:
- output 1: bfloat16 [16384, 512], P('gp')
- output 2: bfloat16 [16384, 512], P('gp')
- output 3: float32 [16384, 474], P('gp')
- output 4: float32 [474, 512], replicated
- output 5: float32 [3, 512], replicated
- output 6: float32 [4, 512], replicated
- output 7: float32 [1536, 512], replicated
- output 8: float32 [1024, 512], replicated
- output 9: float32 [512, 512], replicated
- output 10: float32 [6, 512, 512], replicated
- output 11: float32 [6, 4, 512], replicated
All inputs are finite; a program needn't handle non-finite values.
Results may differ from the reference program's by a relative error of at most 0.0191016.
Values are sent between devices in bfloat16 or wider.
A program may use at most 1 GiB of HBM per device.

```python
import jax
import jax.numpy as jnp
from jax import lax

NUM_PARTS = 32
GRID_DEV = 512
MESH_DEV = 512
FEATURES = 474
LATENT = 512
MESH_FEAT = 3
EDGE_FEAT = 4
EDGE_DEV = 768
SLOT_CAP = 16
GRID_ALL = NUM_PARTS * GRID_DEV
MESH_ALL = NUM_PARTS * MESH_DEV
EDGE_ALL = NUM_PARTS * EDGE_DEV
LN_EPS = 1e-5


def draw_indices(key):
    sub_keys = jax.random.split(key, 5)
    band_ids = jnp.arange(NUM_PARTS)
    polar_band = (band_ids == 0) | (band_ids == NUM_PARTS - 1)
    low_cap = SLOT_CAP // 4
    counts = low_cap + jax.random.randint(sub_keys[0], (NUM_PARTS, NUM_PARTS), 0, SLOT_CAP - low_cap + 1, dtype=jnp.int32)
    counts = jnp.where(polar_band[:, None], SLOT_CAP, counts)
    send_rows = jax.random.randint(sub_keys[1], (NUM_PARTS * NUM_PARTS, SLOT_CAP), 0, GRID_DEV, dtype=jnp.int32)
    slot_valid = jnp.arange(SLOT_CAP)[None, None, :] < counts.T[:, :, None]
    buf_len = NUM_PARTS * SLOT_CAP
    slot_valid = slot_valid.reshape(NUM_PARTS, buf_len)
    order_key = jnp.where(slot_valid, 0, buf_len) + jnp.arange(buf_len)[None, :]
    slot_order = jnp.argsort(order_key, axis=1).astype(jnp.int32)
    n_valid = jnp.sum(slot_valid, axis=1).astype(jnp.int32)
    edge_ids = jnp.arange(EDGE_DEV, dtype=jnp.int32)[None, :]
    slot_pick = jax.random.randint(sub_keys[2], (NUM_PARTS, EDGE_DEV), 0, n_valid[:, None], dtype=jnp.int32)
    slot_pick = jnp.where(edge_ids < n_valid[:, None], edge_ids, slot_pick)
    edge_src = jnp.take_along_axis(slot_order, slot_pick, axis=1)
    dst_draw = jax.random.randint(sub_keys[3], (NUM_PARTS, EDGE_DEV), 0, MESH_DEV, dtype=jnp.int32)
    dst_draw = jnp.where(edge_ids < MESH_DEV, edge_ids, dst_draw)
    edge_dst = jax.random.permutation(sub_keys[4], dst_draw, axis=1, independent=True)
    return send_rows, edge_src.reshape(-1).astype(jnp.int32), edge_dst.reshape(-1).astype(jnp.int32)


def weight_draw(key, shape, fan_in):
    return (jax.random.normal(key, shape, jnp.float32) * fan_in ** -0.5).astype(jnp.bfloat16)


def setup_inputs(seed: int = 0) -> dict:
    key = jax.random.key(seed)
    sub_keys = jax.random.split(key, 16)
    send_rows, edge_src, edge_dst = draw_indices(sub_keys[0])
    grid_in = jax.random.normal(sub_keys[1], (GRID_ALL, FEATURES), jnp.float32)
    lat_draw = jax.random.uniform(sub_keys[2], (MESH_ALL,), jnp.float32, -1.5, 1.5)
    lon_draw = jax.random.uniform(sub_keys[3], (MESH_ALL,), jnp.float32, 0.0, 6.28)
    mesh_static = jnp.stack([jnp.cos(lat_draw), jnp.sin(lon_draw), jnp.cos(lon_draw)], axis=1)
    offsets = 0.5 * jax.random.normal(sub_keys[4], (EDGE_ALL, EDGE_FEAT - 1), jnp.float32)
    lengths = jnp.sqrt(jnp.sum(offsets * offsets, axis=1, keepdims=True))
    edge_static = jnp.concatenate([lengths, offsets], axis=1)
    vec_noise = jax.random.normal(sub_keys[12], (6, 4, LATENT), jnp.float32)
    vec_scale = jnp.array([0.3, 0.3, 0.2, 0.3], jnp.float32)
    vec_shift = jnp.array([0.0, 0.0, 1.0, 0.0], jnp.float32)
    vectors = vec_noise * vec_scale[None, :, None] + vec_shift[None, :, None]
    return {
        'grid_in': grid_in.astype(jnp.bfloat16),
        'mesh_static': mesh_static.astype(jnp.bfloat16),
        'edge_static': edge_static.astype(jnp.bfloat16),
        'send_rows': send_rows,
        'edge_src': edge_src,
        'edge_dst': edge_dst,
        'w_grid_in': weight_draw(sub_keys[5], (FEATURES, LATENT), FEATURES),
        'w_mesh_in': weight_draw(sub_keys[6], (MESH_FEAT, LATENT), MESH_FEAT),
        'w_edge_in': weight_draw(sub_keys[7], (EDGE_FEAT, LATENT), EDGE_FEAT),
        'w_edge_up': weight_draw(sub_keys[8], (3 * LATENT, LATENT), 3 * LATENT),
        'w_mesh_up': weight_draw(sub_keys[9], (2 * LATENT, LATENT), 2 * LATENT),
        'w_grid_up': weight_draw(sub_keys[10], (LATENT, LATENT), LATENT),
        'w_second': weight_draw(sub_keys[11], (6, LATENT, LATENT), LATENT),
        'vectors': vectors,
        'd_mesh_out': jax.random.normal(sub_keys[13], (MESH_ALL, LATENT), jnp.float32).astype(jnp.bfloat16),
        'd_grid_out': jax.random.normal(sub_keys[14], (GRID_ALL, LATENT), jnp.float32).astype(jnp.bfloat16),
    }


def mlp_tail(pre_act, w_two, vec_rows):
    pre_bias = pre_act + vec_rows[0]
    hidden = jax.nn.silu(pre_bias).astype(jnp.bfloat16)
    out_lin = jnp.dot(hidden, w_two, preferred_element_type=jnp.float32) + vec_rows[1]
    centered = out_lin - jnp.mean(out_lin, axis=-1, keepdims=True)
    inv_std = lax.rsqrt(jnp.mean(centered * centered, axis=-1, keepdims=True) + LN_EPS)
    return centered * inv_std * vec_rows[2] + vec_rows[3]


def first_layer(feat_in, w_first):
    return jnp.dot(feat_in, w_first, preferred_element_type=jnp.float32)


def reference(grid_in, mesh_static, edge_static, send_rows, edge_src, edge_dst, w_grid_in, w_mesh_in, w_edge_in, w_edge_up, w_mesh_up, w_grid_up, w_second, vectors, d_mesh_out, d_grid_out):
    edge_part = jnp.arange(EDGE_ALL, dtype=jnp.int32) // EDGE_DEV
    band_ids = edge_src // SLOT_CAP
    sender = band_ids * GRID_DEV + send_rows[band_ids * NUM_PARTS + edge_part, edge_src % SLOT_CAP]
    receiver = edge_part * MESH_DEV + edge_dst

    def forward(grid_x, wg_in, wm_in, we_in, we_up, wm_up, wg_up, w_two_all, vec_all):
        grid_lat = mlp_tail(first_layer(grid_x, wg_in), w_two_all[0], vec_all[0]).astype(jnp.bfloat16)
        mesh_lat = mlp_tail(first_layer(mesh_static, wm_in), w_two_all[1], vec_all[1]).astype(jnp.bfloat16)
        edge_lat = mlp_tail(first_layer(edge_static, we_in), w_two_all[2], vec_all[2]).astype(jnp.bfloat16)
        edge_cat = jnp.concatenate([edge_lat, jnp.take(grid_lat, sender, axis=0), jnp.take(mesh_lat, receiver, axis=0)], axis=1)
        edge_new = (edge_lat.astype(jnp.float32) + mlp_tail(first_layer(edge_cat, we_up), w_two_all[3], vec_all[3])).astype(jnp.bfloat16)
        agg_sum = jax.ops.segment_sum(edge_new.astype(jnp.float32), receiver, num_segments=MESH_ALL)
        mesh_cat = jnp.concatenate([mesh_lat, agg_sum.astype(jnp.bfloat16)], axis=1)
        mesh_out = (mesh_lat.astype(jnp.float32) + mlp_tail(first_layer(mesh_cat, wm_up), w_two_all[4], vec_all[4])).astype(jnp.bfloat16)
        grid_out = (grid_lat.astype(jnp.float32) + mlp_tail(first_layer(grid_lat, wg_up), w_two_all[5], vec_all[5])).astype(jnp.bfloat16)
        return mesh_out, grid_out

    fwd_outs, pull_back = jax.vjp(forward, grid_in, w_grid_in, w_mesh_in, w_edge_in, w_edge_up, w_mesh_up, w_grid_up, w_second, vectors)
    all_grads = pull_back((d_mesh_out, d_grid_out))
    return (fwd_outs[0], fwd_outs[1], all_grads[0].astype(jnp.float32), all_grads[1].astype(jnp.float32), all_grads[2].astype(jnp.float32), all_grads[3].astype(jnp.float32), all_grads[4].astype(jnp.float32), all_grads[5].astype(jnp.float32), all_grads[6].astype(jnp.float32), all_grads[7].astype(jnp.float32), all_grads[8].astype(jnp.float32))
```

```python
import jax
import jax.numpy as jnp
from jax import lax
from jax.experimental import pallas as pl
from jax.experimental.pallas import tpu as pltpu
from jax.sharding import PartitionSpec as P

LN_EPS = 1e-5
AXIS_NAME = 'gp'
NCHUNK = 13
TILE = 256
LATENT = 512
F32 = jnp.float32
BF16 = jnp.bfloat16


def matmul(lhs, rhs):
    return jnp.dot(lhs, rhs, preferred_element_type=jnp.float32)


def contract_rows(lhs, rhs):
    return lax.dot_general(lhs, rhs, (((0,), (0,)), ((), ())), preferred_element_type=jnp.float32)


def contract_cols(lhs, rhs):
    return lax.dot_general(lhs, rhs, (((1,), (1,)), ((), ())), preferred_element_type=jnp.float32)


class Place:
    def __init__(self):
        self.p = lax.axis_index(AXIS_NAME)
        self.c = self.p % 2
        self.x = (self.p // 2) % 2
        self.y = (self.p // 4) % 2
        self.z = self.p // 8
        self.core_peer = self.p + 1 - 2 * self.c
        self.x_peer = self.p + 2 - 4 * self.x
        self.y_peer = self.p + 4 - 8 * self.y

    def z_peer(self, j):
        return self.p % 8 + ((self.z + 1 + j) % 4) * 8


class Reducer:
    def __init__(self, at, grads, out, r0, r1, r2, r3, send, recv):
        self.at = at
        self.grads, self.out = grads, out
        self.r0, self.r1, self.r2, self.r3 = r0, r1, r2, r3
        self.send, self.recv = send, recv

    def spot(self, k):
        at = self.at
        odd = k % 2
        d1 = at.x * (1 - odd) + at.y * odd
        d2 = at.y * (1 - odd) + at.x * odd
        p1 = at.x_peer * (1 - odd) + at.y_peer * odd
        p2 = at.y_peer * (1 - odd) + at.x_peer * odd
        return d1, d2, p1, p2

    def copies(self, s, k):
        at = self.at
        d1, d2, p1, p2 = self.spot(k)

        def make(src, dst, lane, dev):
            return pltpu.make_async_remote_copy(
                src_ref=src, dst_ref=dst, send_sem=self.send.at[k, lane], recv_sem=self.recv.at[k, lane],
                device_id=(dev,), device_id_type=pl.DeviceIdType.MESH)

        def rows(start, size):
            return pl.ds(pl.multiple_of(start, 64), size)

        row1 = at.c * 256 + d1 * 128
        row2 = row1 + d2 * 64
        if s == 0:
            return [make(self.grads.at[k, rows((1 - at.c) * 256, 256)], self.r0.at[k], 0, at.core_peer)]
        if s == 1:
            return [make(self.grads.at[k, rows(at.c * 256 + (1 - d1) * 128, 128)], self.r1.at[k], 1, p1)]
        if s == 2:
            return [make(self.grads.at[k, rows(row1 + (1 - d2) * 64, 64)], self.r2.at[k], 2, p2)]
        if s == 3:
            cols = [pl.ds(pl.multiple_of(((at.z + 1 + j) % 4) * 128, 128), 128) for j in range(3)]
            return [make(self.grads.at[k, rows(row2, 64), cols[j]], self.r3.at[k, j], 3 + j, at.z_peer(j)) for j in range(3)]
        if s == 4:
            part = self.out.at[k, rows(row2, 64), pl.ds(pl.multiple_of(at.z * 128, 128), 128)]
            return [make(part, part, 6 + j, at.z_peer(j)) for j in range(3)]
        if s == 5:
            part = self.out.at[k, rows(row2, 64)]
            return [make(part, part, 9, p2)]
        if s == 6:
            part = self.out.at[k, rows(row1, 128)]
            return [make(part, part, 10, p1)]
        part = self.out.at[k, rows(at.c * 256, 256)]
        return [make(part, part, 11, at.core_peer)]

    def start(self, s, k):
        for copy in self.copies(s, k):
            copy.start()

    def stage(self, s, k):
        at = self.at
        d1, d2, _, _ = self.spot(k)
        for copy in self.copies(s, k):
            copy.wait_recv()
        row1 = at.c * 256 + d1 * 128
        row2 = row1 + d2 * 64
        if s < 3:
            start, size, landed = ((at.c * 256, 256, self.r0), (row1, 128, self.r1), (row2, 64, self.r2))[s]

            @pl.loop(0, size // 64)
            def _(i):
                mine = (k, pl.ds(pl.multiple_of(start + i * 64, 64), 64))
                theirs = landed[k, pl.ds(pl.multiple_of(i * 64, 64), 64)]
                self.grads[mine] = (self.grads[mine].astype(F32) + theirs.astype(F32)).astype(BF16)
        elif s == 3:
            spot = (k, pl.ds(pl.multiple_of(row2, 64), 64), pl.ds(pl.multiple_of(at.z * 128, 128), 128))
            total = self.grads[spot].astype(F32)
            for j in range(3):
                total = total + self.r3[k, j].astype(F32)
            self.out[spot] = total.astype(BF16)
        if s < 7:
            self.start(s + 1, k)

    def drain(self, k):
        for s in range(8):
            for copy in self.copies(s, k):
                copy.wait_send()


class Progress:
    def __init__(self, red):
        self.red, self.now, self.due = red, 0, []

    def ready(self, k):
        self.red.start(0, k)
        self.due += [(self.now + 1 + s, k, s) for s in range(8)]

    def poll(self):
        self.now += 1
        for _, k, s in sorted(d for d in self.due if d[0] <= self.now):
            self.red.stage(s, k)
        self.due = [d for d in self.due if d[0] > self.now]

    def finish(self):
        while self.due:
            self.poll()


def rows_of(i, tile=TILE):
    return pl.ds(pl.multiple_of(i * tile, tile), tile)


def step_kernel(grid_in, mesh_static, edge_static, send_row, src_row, dst_row, w_grid_in, w_mesh_in, w_edge_in, w_edge_up,
                w_mesh_up, w_grid_up, w_second, vectors, d_mesh_out, d_grid_out,
                mesh_out, grid_out, d_grid_in, sums,
                grads, r0, r1, r2, r3, red_send, red_recv, a2a_send, a2a_recv,
                hid0, dsl0, nrm0, inv0, hid1, dsl1, nrm1, inv1, hid2, dsl2, nrm2, inv2, hid3, dsl3, nrm3, inv3,
                hid_s, dlin_s, dpre_s, dlin3, dpre3, dpre4,
                pick_send, pick_src, pick_dst, grid_lat, mesh_lat, cat, edge_new, agg, d_agg, d_edge,
                outgoing, incoming, d_incoming, d_outgoing, d_grid_lat, d_node, d_slot, misc):
    at = Place()
    n_dev = 32
    barrier = pltpu.get_barrier_semaphore()

    @pl.loop(1, n_dev)
    def _(r):
        pl.semaphore_signal(barrier, inc=1, device_id=((at.p + r) % n_dev,), device_id_type=pl.DeviceIdType.MESH)

    red = Reducer(at, grads, sums, r0, r1, r2, r3, red_send, red_recv)
    prog = Progress(red)

    def vec(k, j):
        return vectors[k, pl.ds(j, 1), :]

    def tail(k, pre, rows, hid):
        pre = pre + vec(k, 0)
        sig = jax.nn.sigmoid(pre)
        act = pre * sig
        hid_bf = act.astype(BF16)
        hid[rows, :] = hid_bf
        out_lin = matmul(hid_bf, w_second[k]) + vec(k, 1)
        centered = out_lin - jnp.mean(out_lin, axis=-1, keepdims=True)
        inv = lax.rsqrt(jnp.mean(centered * centered, axis=-1, keepdims=True) + LN_EPS)
        normed = centered * inv
        return normed * vec(k, 2) + vec(k, 3), sig + act * (1.0 - sig), normed, inv

    def tail_saved(k, pre, rows, saves):
        hid, dsl, nrm, inv_ref = saves
        out, slope, normed, inv = tail(k, pre, rows, hid)
        dsl[rows, :] = slope
        nrm[rows, :] = normed
        inv_ref[rows, :] = inv
        return out

    def tail_back(k, d_out, slope, normed, inv, rows, dlin, dpre):
        d_normed = d_out * vec(k, 2)
        d_lin = inv * (d_normed - jnp.mean(d_normed, axis=-1, keepdims=True)
                       - normed * jnp.mean(d_normed * normed, axis=-1, keepdims=True))
        d_lin_bf = d_lin.astype(BF16)
        dlin[rows, :] = d_lin_bf
        d_pre = contract_cols(d_lin_bf, w_second[k]) * slope
        d_pre_bf = d_pre.astype(BF16)
        dpre[rows, :] = d_pre_bf
        for j, term in enumerate((d_pre, d_lin, d_out * normed, d_out)):
            spot = pl.ds(481 + 4 * k + j, 1)
            misc[spot, :] = misc[spot, :] + jnp.sum(term, axis=0, keepdims=True)
        return d_pre_bf

    def tail_back_saved(k, d_out, rows, saves, dlin, dpre):
        _, dsl, nrm, inv_ref = saves
        return tail_back(k, d_out, dsl[rows, :], nrm[rows, :], inv_ref[rows, :], rows, dlin, dpre)

    def weight_grad(k, lhs, rhs, n_rows, first=0):
        @pl.loop(0, LATENT // TILE)
        def _(i):
            cols = pl.ds(pl.multiple_of(first + i * TILE, TILE), TILE)
            part = contract_rows(lhs[pl.ds(0, n_rows), cols], rhs[pl.ds(0, n_rows), :])
            grads[k, rows_of(i), :] = part.astype(BF16)

    def exchange(src, dst, lane, start):
        def copy(r):
            to = (at.p + r) % n_dev
            return pltpu.make_async_remote_copy(
                src_ref=src.at[pl.ds(pl.multiple_of(to * 16, 16), 16)], dst_ref=dst.at[pl.ds(pl.multiple_of(at.p * 16, 16), 16)],
                send_sem=a2a_send.at[lane, r], recv_sem=a2a_recv.at[lane, r],
                device_id=(to,), device_id_type=pl.DeviceIdType.MESH)

        if start:
            @pl.loop(1, n_dev)
            def _(r):
                copy(r).start()

            mine = pl.ds(pl.multiple_of(at.p * 16, 16), 16)
            dst[mine, :] = src[mine, :]
        else:
            @pl.loop(1, n_dev)
            def _(r):
                copy(r).wait()

    saves0 = (hid0, dsl0, nrm0, inv0)
    saves1 = (hid1, dsl1, nrm1, inv1)
    saves2 = (hid2, dsl2, nrm2, inv2)
    saves3 = (hid3, dsl3, nrm3, inv3)
    misc[pl.ds(472, 40), :] = jnp.zeros((40, LATENT), F32)

    @pl.loop(0, 2)
    def _(i):
        rows = rows_of(i)
        out = tail_saved(0, matmul(grid_in[rows, :], w_grid_in[...]), rows, saves0)
        grid_lat[rows, :] = out.astype(BF16)
        ids = lax.broadcasted_iota(jnp.int32, (TILE, LATENT), 0) + i * TILE
        pick_send[rows, :] = jnp.where(ids == send_row[...], 1.0, 0.0).astype(BF16)

    @pl.loop(0, 2)
    def _(i):
        rows = rows_of(i)
        outgoing[rows, :] = contract_rows(pick_send[:, rows], grid_lat[...]).astype(BF16)

    pl.semaphore_wait(barrier, n_dev - 1)
    exchange(outgoing, incoming, 0, True)

    @pl.loop(0, 2)
    def _(i):
        rows = rows_of(i)
        lat = grid_lat[rows, :]
        upd, slope, normed, inv = tail(5, matmul(lat, w_grid_up[...]), rows, hid_s)
        grid_out[rows, :] = (lat.astype(F32) + upd).astype(BF16)
        d_top = d_grid_out[rows, :].astype(F32)
        d_pre = tail_back(5, d_top, slope, normed, inv, rows, dlin_s, dpre_s)
        d_grid_lat[rows, :] = d_top + contract_cols(d_pre, w_grid_up[...])

    weight_grad(0, grid_lat, dpre_s, 512)
    prog.ready(0)
    weight_grad(1, hid_s, dlin_s, 512)
    prog.ready(1)

    @pl.loop(0, 2)
    def _(i):
        rows = rows_of(i)
        out = tail_saved(1, matmul(mesh_static[rows, :], w_mesh_in[...]), rows, saves1)
        mesh_lat[rows, :] = out.astype(BF16)
        ids = lax.broadcasted_iota(jnp.int32, (TILE, 768), 0) + i * TILE
        pick_src[rows, :] = jnp.where(ids == src_row[...], 1.0, 0.0).astype(BF16)
        pick_dst[rows, :] = jnp.where(ids == dst_row[...], 1.0, 0.0).astype(BF16)

    prog.poll()

    @pl.loop(0, 3)
    def _(i):
        rows = rows_of(i)
        out = tail_saved(2, matmul(edge_static[rows, :], w_edge_in[...]), rows, saves2)
        cat[rows, pl.ds(0, 512)] = out.astype(BF16)
        cat[rows, pl.ds(1024, 512)] = contract_rows(pick_dst[:, rows], mesh_lat[...]).astype(BF16)

    prog.poll()
    exchange(outgoing, incoming, 0, False)

    @pl.loop(0, 3)
    def _(i):
        rows = rows_of(i)
        cat[rows, pl.ds(512, 512)] = contract_rows(pick_src[:, rows], incoming[...]).astype(BF16)
        upd = tail_saved(3, matmul(cat[rows, :], w_edge_up[...]), rows, saves3)
        edge_new[rows, :] = (cat[rows, pl.ds(0, 512)].astype(F32) + upd).astype(BF16)

    prog.poll()

    @pl.loop(0, 2)
    def _(i):
        rows = rows_of(i)
        lat = mesh_lat[rows, :]
        agg_bf = matmul(pick_dst[rows, :], edge_new[...]).astype(BF16)
        agg[rows, :] = agg_bf
        pre = matmul(lat, w_mesh_up[pl.ds(0, 512), :]) + matmul(agg_bf, w_mesh_up[pl.ds(512, 512), :])
        upd, slope, normed, inv = tail(4, pre, rows, hid_s)
        mesh_out[rows, :] = (lat.astype(F32) + upd).astype(BF16)
        d_pre = tail_back(4, d_mesh_out[rows, :].astype(F32), slope, normed, inv, rows, dlin_s, dpre4)
        d_agg[rows, :] = contract_cols(d_pre, w_mesh_up[pl.ds(512, 512), :]).astype(BF16)

    prog.poll()

    @pl.loop(0, 3)
    def _(i):
        rows = rows_of(i)
        d_out = contract_rows(pick_dst[:, rows], d_agg[...])
        d_edge[rows, :] = d_out.astype(BF16)
        tail_back_saved(3, d_out, rows, saves3, dlin3, dpre3)

    prog.poll()

    @pl.loop(0, 2)
    def _(i):
        rows = rows_of(i)
        slot = matmul(pick_src[rows, :], dpre3[...]).astype(BF16)
        d_incoming[rows, :] = contract_cols(slot, w_edge_up[pl.ds(512, 512), :]).astype(BF16)

    exchange(d_incoming, d_outgoing, 1, True)
    weight_grad(2, mesh_lat, dpre4, 512)
    prog.ready(2)
    weight_grad(3, agg, dpre4, 512)
    prog.ready(3)
    weight_grad(4, hid_s, dlin_s, 512)
    prog.ready(4)
    prog.poll()
    for part in range(3):
        weight_grad(5 + part, cat, dpre3, 768, first=512 * part)
        prog.ready(5 + part)
    weight_grad(8, hid3, dlin3, 768)
    prog.ready(8)
    prog.poll()

    @pl.loop(0, 3)
    def _(i):
        rows = rows_of(i)
        d_out = d_edge[rows, :].astype(F32) + contract_cols(dpre3[rows, :], w_edge_up[pl.ds(0, 512), :])
        tail_back_saved(2, d_out, rows, saves2, dlin_s, dpre_s)

    weight_grad(9, hid2, dlin_s, 768)
    misc[pl.ds(477, 4), :] = contract_rows(edge_static[...], dpre_s[...])
    prog.ready(9)
    prog.poll()

    @pl.loop(0, 2)
    def _(i):
        rows = rows_of(i)
        node = matmul(pick_dst[rows, :], dpre3[...]).astype(BF16)
        d_out = (d_mesh_out[rows, :].astype(F32) + contract_cols(dpre4[rows, :], w_mesh_up[pl.ds(0, 512), :])
                 + contract_cols(node, w_edge_up[pl.ds(1024, 512), :]))
        tail_back_saved(1, d_out, rows, saves1, dlin_s, dpre_s)

    weight_grad(10, hid1, dlin_s, 512)
    misc[pl.ds(474, 3), :] = contract_rows(mesh_static[...], dpre_s[pl.ds(0, 512), :])
    prog.ready(10)
    prog.poll()
    exchange(d_incoming, d_outgoing, 1, False)

    @pl.loop(0, 2)
    def _(i):
        rows = rows_of(i)
        d_out = d_grid_lat[rows, :] + matmul(pick_send[rows, :], d_outgoing[...])
        d_pre = tail_back_saved(0, d_out, rows, saves0, dlin_s, dpre_s)
        d_grid_in[rows, :] = contract_cols(d_pre, w_grid_in[...])

    weight_grad(12, hid0, dlin_s, 512)
    prog.ready(12)
    misc[pl.ds(0, 474), :] = contract_rows(grid_in[...], dpre_s[pl.ds(0, 512), :])
    grads[11] = misc[...].astype(BF16)
    prog.ready(11)
    prog.finish()

    @pl.loop(0, NCHUNK)
    def _(k):
        red.drain(k)


def fused_step(*args):
    def f32(*shape):
        return pltpu.VMEM(shape, F32)

    def bf16(*shape):
        return pltpu.VMEM(shape, BF16)

    def saves(n):
        return [bf16(n, 512), f32(n, 512), f32(n, 512), f32(n, 1)]

    scratch = [
        bf16(NCHUNK, 512, 512), bf16(NCHUNK, 256, 512), bf16(NCHUNK, 128, 512), bf16(NCHUNK, 64, 512), bf16(NCHUNK, 3, 64, 128),
        pltpu.SemaphoreType.DMA((NCHUNK, 12)), pltpu.SemaphoreType.DMA((NCHUNK, 12)),
        pltpu.SemaphoreType.DMA((2, 32)), pltpu.SemaphoreType.DMA((2, 32)),
        *saves(512), *saves(512), *saves(768), *saves(768),
        bf16(768, 512), bf16(768, 512), bf16(768, 512), bf16(768, 512), bf16(768, 512), bf16(512, 512),
        bf16(512, 512), bf16(512, 768), bf16(512, 768), bf16(512, 512), bf16(512, 512), bf16(768, 1536), bf16(768, 512),
        bf16(512, 512), bf16(512, 512), bf16(768, 512),
        bf16(512, 512), bf16(512, 512), bf16(512, 512), bf16(512, 512), f32(512, 512), bf16(8, 512), bf16(8, 512), f32(512, 512),
    ]
    return pl.pallas_call(
        step_kernel,
        out_shape=[jax.ShapeDtypeStruct((512, 512), BF16), jax.ShapeDtypeStruct((512, 512), BF16),
                   jax.ShapeDtypeStruct((512, 474), F32), jax.ShapeDtypeStruct((NCHUNK, 512, 512), BF16)],
        in_specs=[pl.BlockSpec(memory_space=pltpu.VMEM)] * len(args),
        out_specs=[pl.BlockSpec(memory_space=pltpu.VMEM)] * 4,
        scratch_shapes=scratch,
        compiler_params=pltpu.CompilerParams(collective_id=0, has_side_effects=True, vmem_limit_bytes=67043328),
    )(*args)


def solution(mesh):
    row_spec = P(AXIS_NAME, None)
    edge_spec = P(AXIS_NAME)
    rep_spec = P()
    in_specs = (row_spec, row_spec, row_spec, row_spec, edge_spec, edge_spec) + (rep_spec,) * 8 + (row_spec, row_spec)
    out_specs = (row_spec, row_spec, row_spec) + (rep_spec,) * 8

    def local_step(grid_in, mesh_static, edge_static, send_rows, edge_src, edge_dst, *rest):
        mesh_out, grid_out, d_grid_in, total = fused_step(
            grid_in, mesh_static, edge_static, send_rows.reshape(1, -1), edge_src.reshape(1, -1), edge_dst.reshape(1, -1), *rest)
        misc = total[11]
        weight_sums = (misc[:474], misc[474:477], misc[477:481], total[5:8].reshape(1536, 512), total[2:4].reshape(1024, 512),
                       total[0], jnp.stack([total[k] for k in (12, 10, 9, 8, 4, 1)]), misc[481:505].reshape(6, 4, 512))
        return (mesh_out, grid_out, d_grid_in) + tuple(part.astype(F32) for part in weight_sums)

    return jax.shard_map(local_step, mesh=mesh, in_specs=in_specs, out_specs=out_specs, check_vma=False)
```

```python
import jax
import jax.numpy as jnp
from jax import lax
from jax.experimental import pallas as pl
from jax.experimental.pallas import tpu as pltpu
from jax.sharding import PartitionSpec as P

LN_EPS = 1e-5
AXIS_NAME = 'gp'
NCHUNK = 13
TILE = 256
LATENT = 512
F32 = jnp.float32
BF16 = jnp.bfloat16


def matmul(lhs, rhs):
    return jnp.dot(lhs, rhs, preferred_element_type=jnp.float32)


def contract_rows(lhs, rhs):
    return lax.dot_general(lhs, rhs, (((0,), (0,)), ((), ())), preferred_element_type=jnp.float32)


def contract_cols(lhs, rhs):
    return lax.dot_general(lhs, rhs, (((1,), (1,)), ((), ())), preferred_element_type=jnp.float32)


class Place:
    def __init__(self):
        self.p = lax.axis_index(AXIS_NAME)
        self.c = self.p % 2
        self.x = (self.p // 2) % 2
        self.y = (self.p // 4) % 2
        self.z = self.p // 8
        self.core_peer = self.p + 1 - 2 * self.c
        self.x_peer = self.p + 2 - 4 * self.x
        self.y_peer = self.p + 4 - 8 * self.y

    def z_peer(self, j):
        return self.p % 8 + ((self.z + 1 + j) % 4) * 8


class Reducer:
    def __init__(self, at, grads, out, r0, r1, r2, r3, send, recv):
        self.at = at
        self.grads, self.out = grads, out
        self.r0, self.r1, self.r2, self.r3 = r0, r1, r2, r3
        self.send, self.recv = send, recv

    def spot(self, k):
        at = self.at
        odd = k % 2
        d1 = at.x * (1 - odd) + at.y * odd
        d2 = at.y * (1 - odd) + at.x * odd
        p1 = at.x_peer * (1 - odd) + at.y_peer * odd
        p2 = at.y_peer * (1 - odd) + at.x_peer * odd
        return d1, d2, p1, p2

    def copies(self, s, k):
        at = self.at
        d1, d2, p1, p2 = self.spot(k)

        def make(src, dst, lane, dev):
            return pltpu.make_async_remote_copy(
                src_ref=src, dst_ref=dst, send_sem=self.send.at[k, lane], recv_sem=self.recv.at[k, lane],
                device_id=(dev,), device_id_type=pl.DeviceIdType.MESH)

        def rows(start, size):
            return pl.ds(pl.multiple_of(start, 64), size)

        row1 = at.c * 256 + d1 * 128
        row2 = row1 + d2 * 64
        if s == 0:
            return [make(self.grads.at[k, rows((1 - at.c) * 256, 256)], self.r0.at[k], 0, at.core_peer)]
        if s == 1:
            return [make(self.grads.at[k, rows(at.c * 256 + (1 - d1) * 128, 128)], self.r1.at[k], 1, p1)]
        if s == 2:
            return [make(self.grads.at[k, rows(row1 + (1 - d2) * 64, 64)], self.r2.at[k], 2, p2)]
        if s == 3:
            cols = [pl.ds(pl.multiple_of(((at.z + 1 + j) % 4) * 128, 128), 128) for j in range(3)]
            return [make(self.grads.at[k, rows(row2, 64), cols[j]], self.r3.at[k, j], 3 + j, at.z_peer(j)) for j in range(3)]
        if s == 4:
            part = self.out.at[k, rows(row2, 64), pl.ds(pl.multiple_of(at.z * 128, 128), 128)]
            return [make(part, part, 6 + j, at.z_peer(j)) for j in range(3)]
        if s == 5:
            part = self.out.at[k, rows(row2, 64)]
            return [make(part, part, 9, p2)]
        if s == 6:
            part = self.out.at[k, rows(row1, 128)]
            return [make(part, part, 10, p1)]
        part = self.out.at[k, rows(at.c * 256, 256)]
        return [make(part, part, 11, at.core_peer)]

    def start(self, s, k):
        for copy in self.copies(s, k):
            copy.start()

    def stage(self, s, k):
        at = self.at
        d1, d2, _, _ = self.spot(k)
        for copy in self.copies(s, k):
            copy.wait_recv()
        row1 = at.c * 256 + d1 * 128
        row2 = row1 + d2 * 64
        if s < 3:
            start, size, landed = ((at.c * 256, 256, self.r0), (row1, 128, self.r1), (row2, 64, self.r2))[s]

            @pl.loop(0, size // 64)
            def _(i):
                mine = (k, pl.ds(pl.multiple_of(start + i * 64, 64), 64))
                theirs = landed[k, pl.ds(pl.multiple_of(i * 64, 64), 64)]
                self.grads[mine] = (self.grads[mine].astype(F32) + theirs.astype(F32)).astype(BF16)
        elif s == 3:
            spot = (k, pl.ds(pl.multiple_of(row2, 64), 64), pl.ds(pl.multiple_of(at.z * 128, 128), 128))
            total = self.grads[spot].astype(F32)
            for j in range(3):
                total = total + self.r3[k, j].astype(F32)
            self.out[spot] = total.astype(BF16)
        if s < 7:
            self.start(s + 1, k)

    def drain(self, k):
        for s in range(8):
            for copy in self.copies(s, k):
                copy.wait_send()


ORDER = (
        (),
        (),
        (),
        (),
        (),
        (0, 1, 16, 17),
        (32, 33),
        (),
        (48,),
        (),
        (49,),
        (),
        (),
        (),
        (),
        (2,),
        (),
        (3, 64, 4, 5),
        (6,),
        (7, 8, 9),
        (18, 19, 80, 10, 20, 21),
        (22, 65),
        (),
        (23, 24, 12, 11, 35, 25, 34, 36, 96, 38, 51, 112, 40, 26, 50, 37, 52, 27, 81, 54, 42, 39, 67, 56, 28, 66, 97,
     41, 53, 113, 43, 68, 44, 83, 70, 82, 58, 84, 55, 72, 99, 98, 57, 86, 115, 69, 88, 114, 100, 59, 60, 116, 102, 74,
     85, 71, 118, 73, 90, 104, 75, 87, 76, 120, 101, 89, 117, 106, 103, 91, 92, 122, 119, 105, 108, 121, 107, 124, 123),
)


class Progress:
    def __init__(self, red):
        self.red, self.point = red, 0

    def ready(self, k):
        self.red.start(0, k)

    def poll(self):
        for code in ORDER[self.point]:
            self.red.stage(code // 16, code % 16)
        self.point += 1


def rows_of(i, tile=TILE):
    return pl.ds(pl.multiple_of(i * tile, tile), tile)


def step_kernel(grid_t, mesh_t, edge_t, send_t, src_row, dst_row, w_grid_in, w_mesh_in, w_edge_in, w_edge_up,
                w_mesh_up, w_grid_up, w_second, vectors, d_mesh_out, d_grid_out,
                mesh_out, grid_out, d_grid_t, sums,
                grads, r0, r1, r2, r3, red_send, red_recv, a2a_send, a2a_recv,
                hid0, dsl0, nrm0, inv0, hid1, dsl1, nrm1, inv1, hid2, dsl2, nrm2, inv2, hid3, dsl3, nrm3, inv3,
                hid_s, dlin_s, dpre_s, dlin3, dpre3, dpre4,
                pick_send, pick_src, pick_dst, grid_lat, mesh_lat, cat, edge_new, agg, d_agg, d_edge,
                outgoing, incoming, d_incoming, d_outgoing, d_grid_lat, d_node, d_slot, misc):
    at = Place()
    n_dev = 32
    barrier = pltpu.get_barrier_semaphore()

    @pl.loop(1, n_dev)
    def _(r):
        pl.semaphore_signal(barrier, inc=1, device_id=((at.p + r) % n_dev,), device_id_type=pl.DeviceIdType.MESH)

    red = Reducer(at, grads, sums, r0, r1, r2, r3, red_send, red_recv)
    prog = Progress(red)

    def vec(k, j):
        return vectors[k, pl.ds(j, 1), :]

    def tail(k, pre, rows, hid):
        pre = pre + vec(k, 0)
        sig = jax.nn.sigmoid(pre)
        act = pre * sig
        hid_bf = act.astype(BF16)
        hid[rows, :] = hid_bf
        out_lin = matmul(hid_bf, w_second[k]) + vec(k, 1)
        centered = out_lin - jnp.mean(out_lin, axis=-1, keepdims=True)
        inv = lax.rsqrt(jnp.mean(centered * centered, axis=-1, keepdims=True) + LN_EPS)
        normed = centered * inv
        return normed * vec(k, 2) + vec(k, 3), sig + act * (1.0 - sig), normed, inv

    def tail_saved(k, pre, rows, saves):
        hid, dsl, nrm, inv_ref = saves
        out, slope, normed, inv = tail(k, pre, rows, hid)
        dsl[rows, :] = slope
        nrm[rows, :] = normed
        inv_ref[rows, :] = inv
        return out

    def tail_back(k, d_out, slope, normed, inv, rows, dlin, dpre):
        d_normed = d_out * vec(k, 2)
        d_lin = inv * (d_normed - jnp.mean(d_normed, axis=-1, keepdims=True)
                       - normed * jnp.mean(d_normed * normed, axis=-1, keepdims=True))
        d_lin_bf = d_lin.astype(BF16)
        dlin[rows, :] = d_lin_bf
        d_pre = contract_cols(d_lin_bf, w_second[k]) * slope
        d_pre_bf = d_pre.astype(BF16)
        dpre[rows, :] = d_pre_bf
        for j, term in enumerate((d_pre, d_lin, d_out * normed, d_out)):
            spot = pl.ds(481 + 4 * k + j, 1)
            misc[spot, :] = misc[spot, :] + jnp.sum(term, axis=0, keepdims=True)
        return d_pre_bf

    def tail_back_saved(k, d_out, rows, saves, dlin, dpre):
        _, dsl, nrm, inv_ref = saves
        return tail_back(k, d_out, dsl[rows, :], nrm[rows, :], inv_ref[rows, :], rows, dlin, dpre)

    def weight_grad(k, lhs, rhs, n_rows, first=0):
        @pl.loop(0, LATENT // TILE)
        def _(i):
            cols = pl.ds(pl.multiple_of(first + i * TILE, TILE), TILE)
            part = contract_rows(lhs[pl.ds(0, n_rows), cols], rhs[pl.ds(0, n_rows), :])
            grads[k, rows_of(i), :] = part.astype(BF16)

    def exchange(src, dst, lane, start):
        def copy(r):
            to = (at.p + r) % n_dev
            return pltpu.make_async_remote_copy(
                src_ref=src.at[pl.ds(pl.multiple_of(to * 16, 16), 16)], dst_ref=dst.at[pl.ds(pl.multiple_of(at.p * 16, 16), 16)],
                send_sem=a2a_send.at[lane, r], recv_sem=a2a_recv.at[lane, r],
                device_id=(to,), device_id_type=pl.DeviceIdType.MESH)

        if start:
            @pl.loop(1, n_dev)
            def _(r):
                copy(r).start()

            mine = pl.ds(pl.multiple_of(at.p * 16, 16), 16)
            dst[mine, :] = src[mine, :]
        else:
            @pl.loop(1, n_dev)
            def _(r):
                copy(r).wait()

    saves0 = (hid0, dsl0, nrm0, inv0)
    saves1 = (hid1, dsl1, nrm1, inv1)
    saves2 = (hid2, dsl2, nrm2, inv2)
    saves3 = (hid3, dsl3, nrm3, inv3)
    misc[pl.ds(472, 40), :] = jnp.zeros((40, LATENT), F32)

    def tiles(n):
        def run(body):
            prog.poll()

            @pl.loop(0, n)
            def _(i):
                body(i, rows_of(i))
        return run

    slots = send_t[...]
    spread = jnp.where(lax.broadcasted_iota(jnp.int32, (32, 512), 0) == lax.broadcasted_iota(jnp.int32, (32, 512), 1) // 16,
                       1.0, 0.0).astype(BF16)
    slots = (matmul((slots // 32).astype(F32).astype(BF16), spread) * 32.0
             + matmul((slots % 32).astype(F32).astype(BF16), spread))
    own = lax.broadcasted_iota(jnp.int32, (16, 512), 0) == lax.broadcasted_iota(jnp.int32, (16, 512), 1) % 16
    send_row = jnp.sum(jnp.where(own, slots, 0.0), axis=0, keepdims=True)

    def pick(row, i):
        ids = lax.broadcasted_iota(jnp.int32, (TILE, row.shape[1]), 0) + i * TILE
        return jnp.where(ids == row, 1.0, 0.0).astype(BF16)

    send_ids = send_row.astype(jnp.int32)
    for i in range(2):
        pick_send[rows_of(i), :] = pick(send_ids, i)

    @pl.loop(0, 2)
    def _(i):
        rows = rows_of(i)
        out = tail_saved(0, contract_rows(grid_t[:, rows], w_grid_in[...]), rows, saves0)
        grid_lat[rows, :] = out.astype(BF16)

    @pl.loop(0, 2)
    def _(i):
        rows = rows_of(i)
        outgoing[rows, :] = contract_rows(pick_send[:, rows], grid_lat[...]).astype(BF16)

    pl.semaphore_wait(barrier, n_dev - 1)
    exchange(outgoing, incoming, 0, True)

    @tiles(2)
    def _(i, rows):
        lat = grid_lat[rows, :]
        upd, slope, normed, inv = tail(5, matmul(lat, w_grid_up[...]), rows, hid_s)
        grid_out[rows, :] = (lat.astype(F32) + upd).astype(BF16)
        d_top = d_grid_out[rows, :].astype(F32)
        d_pre = tail_back(5, d_top, slope, normed, inv, rows, dlin_s, dpre_s)
        d_grid_lat[rows, :] = d_top + contract_cols(d_pre, w_grid_up[...])

    def grad(k, *args, **kwargs):
        prog.poll()
        weight_grad(k, *args, **kwargs)
        prog.ready(k)

    grad(0, grid_lat, dpre_s, 512)
    grad(1, hid_s, dlin_s, 512)

    @tiles(2)
    def _(i, rows):
        out = tail_saved(1, contract_rows(mesh_t[:, rows], w_mesh_in[...]), rows, saves1)
        mesh_lat[rows, :] = out.astype(BF16)
        pick_src[rows, :] = pick(src_row[...], i)
        pick_dst[rows, :] = pick(dst_row[...], i)

    @tiles(3)
    def _(i, rows):
        out = tail_saved(2, contract_rows(edge_t[:, rows], w_edge_in[...]), rows, saves2)
        cat[rows, pl.ds(0, 512)] = out.astype(BF16)
        cat[rows, pl.ds(1024, 512)] = contract_rows(pick_dst[:, rows], mesh_lat[...]).astype(BF16)

    prog.poll()
    exchange(outgoing, incoming, 0, False)

    @pl.loop(0, 3)
    def _(i):
        rows = rows_of(i)
        cat[rows, pl.ds(512, 512)] = contract_rows(pick_src[:, rows], incoming[...]).astype(BF16)
        upd = tail_saved(3, matmul(cat[rows, :], w_edge_up[...]), rows, saves3)
        edge_new[rows, :] = (cat[rows, pl.ds(0, 512)].astype(F32) + upd).astype(BF16)

    @tiles(2)
    def _(i, rows):
        lat = mesh_lat[rows, :]
        agg_bf = matmul(pick_dst[rows, :], edge_new[...]).astype(BF16)
        agg[rows, :] = agg_bf
        pre = matmul(lat, w_mesh_up[pl.ds(0, 512), :]) + matmul(agg_bf, w_mesh_up[pl.ds(512, 512), :])
        upd, slope, normed, inv = tail(4, pre, rows, hid_s)
        mesh_out[rows, :] = (lat.astype(F32) + upd).astype(BF16)
        d_pre = tail_back(4, d_mesh_out[rows, :].astype(F32), slope, normed, inv, rows, dlin_s, dpre4)
        d_agg[rows, :] = contract_cols(d_pre, w_mesh_up[pl.ds(512, 512), :]).astype(BF16)

    @tiles(3)
    def _(i, rows):
        d_out = contract_rows(pick_dst[:, rows], d_agg[...])
        d_edge[rows, :] = d_out.astype(BF16)
        tail_back_saved(3, d_out, rows, saves3, dlin3, dpre3)

    @tiles(2)
    def _(i, rows):
        slot = matmul(pick_src[rows, :], dpre3[...]).astype(BF16)
        d_incoming[rows, :] = contract_cols(slot, w_edge_up[pl.ds(512, 512), :]).astype(BF16)

    exchange(d_incoming, d_outgoing, 1, True)
    grad(2, mesh_lat, dpre4, 512)
    grad(3, agg, dpre4, 512)
    grad(4, hid_s, dlin_s, 512)
    for part in range(3):
        grad(5 + part, cat, dpre3, 768, first=512 * part)
    grad(8, hid3, dlin3, 768)

    @tiles(3)
    def _(i, rows):
        d_out = d_edge[rows, :].astype(F32) + contract_cols(dpre3[rows, :], w_edge_up[pl.ds(0, 512), :])
        tail_back_saved(2, d_out, rows, saves2, dlin_s, dpre_s)

    misc[pl.ds(477, 4), :] = matmul(edge_t[...], dpre_s[...])
    grad(9, hid2, dlin_s, 768)

    @tiles(2)
    def _(i, rows):
        node = matmul(pick_dst[rows, :], dpre3[...]).astype(BF16)
        d_out = (d_mesh_out[rows, :].astype(F32) + contract_cols(dpre4[rows, :], w_mesh_up[pl.ds(0, 512), :])
                 + contract_cols(node, w_edge_up[pl.ds(1024, 512), :]))
        tail_back_saved(1, d_out, rows, saves1, dlin_s, dpre_s)

    misc[pl.ds(474, 3), :] = matmul(mesh_t[...], dpre_s[pl.ds(0, 512), :])
    grad(10, hid1, dlin_s, 512)
    prog.poll()
    exchange(d_incoming, d_outgoing, 1, False)

    @pl.loop(0, 2)
    def _(i):
        rows = rows_of(i)
        d_out = d_grid_lat[rows, :] + matmul(pick_send[rows, :], d_outgoing[...])
        d_pre = tail_back_saved(0, d_out, rows, saves0, dlin_s, dpre_s)
        d_grid_t[:, rows] = contract_cols(w_grid_in[...], d_pre)

    grad(12, hid0, dlin_s, 512)
    prog.poll()
    misc[pl.ds(0, 474), :] = matmul(grid_t[...], dpre_s[pl.ds(0, 512), :])
    grads[11] = misc[...].astype(BF16)
    prog.ready(11)
    prog.poll()

    @pl.loop(0, NCHUNK)
    def _(k):
        red.drain(k)


def fused_step(*args):
    def f32(*shape):
        return pltpu.VMEM(shape, F32)

    def bf16(*shape):
        return pltpu.VMEM(shape, BF16)

    def saves(n):
        return [bf16(n, 512), f32(n, 512), f32(n, 512), f32(n, 1)]

    scratch = [
        bf16(NCHUNK, 512, 512), bf16(NCHUNK, 256, 512), bf16(NCHUNK, 128, 512), bf16(NCHUNK, 64, 512), bf16(NCHUNK, 3, 64, 128),
        pltpu.SemaphoreType.DMA((NCHUNK, 12)), pltpu.SemaphoreType.DMA((NCHUNK, 12)),
        pltpu.SemaphoreType.DMA((2, 32)), pltpu.SemaphoreType.DMA((2, 32)),
        *saves(512), *saves(512), *saves(768), *saves(768),
        bf16(768, 512), bf16(768, 512), bf16(768, 512), bf16(768, 512), bf16(768, 512), bf16(512, 512),
        bf16(512, 512), bf16(512, 768), bf16(512, 768), bf16(512, 512), bf16(512, 512), bf16(768, 1536), bf16(768, 512),
        bf16(512, 512), bf16(512, 512), bf16(768, 512),
        bf16(512, 512), bf16(512, 512), bf16(512, 512), bf16(512, 512), f32(512, 512), bf16(8, 512), bf16(8, 512), f32(512, 512),
    ]
    return pl.pallas_call(
        step_kernel,
        out_shape=[jax.ShapeDtypeStruct((512, 512), BF16), jax.ShapeDtypeStruct((512, 512), BF16),
                   jax.ShapeDtypeStruct((474, 512), F32), jax.ShapeDtypeStruct((NCHUNK, 512, 512), BF16)],
        in_specs=[pl.BlockSpec(memory_space=pltpu.VMEM)] * len(args),
        out_specs=[pl.BlockSpec(memory_space=pltpu.VMEM)] * 4,
        scratch_shapes=scratch,
        compiler_params=pltpu.CompilerParams(collective_id=0, has_side_effects=True, vmem_limit_bytes=67043328),
    )(*args)


HOME = {0: (2, 0), 1: (3, 5), 2: (1, 0), 3: (1, 1), 4: (3, 4), 5: (0, 0), 6: (0, 1), 7: (0, 2), 8: (3, 3), 9: (3, 2), 10: (3, 1), 12: (3, 0)}


def spread_kernel(mesh_in, grid_in, d_grid_in, sums, mesh_out, grid_out, d_grid_out, edge_up, mesh_up, grid_up, second,
                  w_grid, w_mesh, w_edge, vecs, mesh_buf, grid_buf, d_grid_buf, sum_buf, wide, sem_in, sem_out):
    loads = [pltpu.make_async_copy(sums.at[k], sum_buf.at[k], sem_in.at[k]) for k in range(NCHUNK)]
    through = [(mesh_in, mesh_buf, mesh_out), (grid_in, grid_buf, grid_out), (d_grid_in, d_grid_buf, d_grid_out)]
    heads = [pltpu.make_async_copy(a, b, sem_in.at[NCHUNK + i]) for i, (a, b, _) in enumerate(through)]
    tails = [pltpu.make_async_copy(b, c, sem_out.at[NCHUNK + i]) for i, (_, b, c) in enumerate(through)]
    loads[11].start()
    for k in range(NCHUNK):
        if k != 11:
            loads[k].start()
    for copy in heads:
        copy.start()
    outs = (edge_up, mesh_up, grid_up, second)
    stores = []
    loads[11].wait()
    misc = sum_buf[11].astype(F32)
    w_grid[...] = misc[:474]
    w_mesh[...] = misc[474:477]
    w_edge[...] = misc[477:481]
    for k in range(6):
        vecs[k] = misc[481 + 4 * k:485 + 4 * k]
    for k, (out, part) in HOME.items():
        loads[k].wait()

        @pl.loop(0, 8)
        def _(i):
            rows = rows_of(i, 64)
            wide[k, rows, :] = sum_buf[k, rows, :].astype(F32)

        home = outs[out].at[part] if out == 3 else outs[out].at[pl.ds(part * 512, 512)]
        stores.append(pltpu.make_async_copy(wide.at[k], home, sem_out.at[k]))
        stores[-1].start()
    for head, tail in zip(heads, tails):
        head.wait()
        tail.start()
    for copy in stores + tails:
        copy.wait()


def spread_out(*parts):
    def out(dtype, *shape):
        return jax.ShapeDtypeStruct(shape, dtype)

    anywhere = pl.BlockSpec(memory_space=pl.ANY)
    here = pl.BlockSpec(memory_space=pltpu.VMEM)
    mesh_out, grid_out, d_grid, edge_up, mesh_up, grid_up, second, w_grid, w_mesh, w_edge, vecs = pl.pallas_call(
        spread_kernel,
        out_shape=[out(BF16, 512, 512), out(BF16, 512, 512), out(F32, 474, 512), out(F32, 1536, 512), out(F32, 1024, 512),
                   out(F32, 512, 512), out(F32, 6, 512, 512), out(F32, 474, 512), out(F32, 3, 512), out(F32, 4, 512),
                   out(F32, 6, 4, 512)],
        in_specs=[anywhere] * 4,
        out_specs=[anywhere] * 7 + [here] * 4,
        scratch_shapes=[pltpu.VMEM((512, 512), BF16), pltpu.VMEM((512, 512), BF16), pltpu.VMEM((474, 512), F32),
                        pltpu.VMEM((NCHUNK, 512, 512), BF16), pltpu.VMEM((NCHUNK, 512, 512), F32),
                        pltpu.SemaphoreType.DMA((NCHUNK + 3,)), pltpu.SemaphoreType.DMA((NCHUNK + 3,))],
        compiler_params=pltpu.CompilerParams(vmem_limit_bytes=48 * 2**20),
    )(*parts)
    return mesh_out, grid_out, d_grid, w_grid, w_mesh, w_edge, edge_up, mesh_up, grid_up, second, vecs


def solution(mesh):
    row_spec = P(AXIS_NAME, None)
    edge_spec = P(AXIS_NAME)
    rep_spec = P()
    in_specs = (row_spec, row_spec, row_spec, row_spec, edge_spec, edge_spec) + (rep_spec,) * 8 + (row_spec, row_spec)
    out_specs = (row_spec, row_spec, row_spec) + (rep_spec,) * 8

    def local_step(grid_in, mesh_static, edge_static, send_rows, edge_src, edge_dst, *rest):
        parts = fused_step(grid_in.T, mesh_static.T, edge_static.T, send_rows.T,
                           edge_src.reshape(1, -1), edge_dst.reshape(1, -1), *rest)
        mesh_out, grid_out, d_grid_t, *sums = spread_out(*parts)
        return (mesh_out, grid_out, d_grid_t.T) + tuple(sums)

    return jax.shard_map(local_step, mesh=mesh, in_specs=in_specs, out_specs=out_specs, check_vma=False)
```

```python
import jax
import jax.numpy as jnp
from jax import lax
from jax.experimental import pallas as pl
from jax.experimental.pallas import tpu as pltpu
from jax.sharding import PartitionSpec as P

LN_EPS = 1e-5
AXIS_NAME = 'gp'
NCHUNK = 13
TILE = 256
LATENT = 512
F32 = jnp.float32
BF16 = jnp.bfloat16


def matmul(lhs, rhs):
    return jnp.dot(lhs, rhs, preferred_element_type=jnp.float32)


def contract_rows(lhs, rhs):
    return lax.dot_general(lhs, rhs, (((0,), (0,)), ((), ())), preferred_element_type=jnp.float32)


def contract_cols(lhs, rhs):
    return lax.dot_general(lhs, rhs, (((1,), (1,)), ((), ())), preferred_element_type=jnp.float32)


class Place:
    def __init__(self):
        self.p = lax.axis_index(AXIS_NAME)
        self.c = self.p % 2
        self.x = (self.p // 2) % 2
        self.y = (self.p // 4) % 2
        self.z = self.p // 8
        self.core_peer = self.p + 1 - 2 * self.c
        self.x_peer = self.p + 2 - 4 * self.x
        self.y_peer = self.p + 4 - 8 * self.y

    def z_peer(self, j):
        return self.p % 8 + ((self.z + 1 + j) % 4) * 8


class Reducer:
    def __init__(self, at, grads, out, r0, r1, r2, r3, send, recv):
        self.at = at
        self.grads, self.out = grads, out
        self.r0, self.r1, self.r2, self.r3 = r0, r1, r2, r3
        self.send, self.recv = send, recv

    def spot(self, k):
        at = self.at
        odd = k % 2
        d1 = at.x * (1 - odd) + at.y * odd
        d2 = at.y * (1 - odd) + at.x * odd
        p1 = at.x_peer * (1 - odd) + at.y_peer * odd
        p2 = at.y_peer * (1 - odd) + at.x_peer * odd
        return d1, d2, p1, p2

    def copies(self, s, k):
        at = self.at
        d1, d2, p1, p2 = self.spot(k)

        def make(src, dst, lane, dev):
            return pltpu.make_async_remote_copy(
                src_ref=src, dst_ref=dst, send_sem=self.send.at[k, lane], recv_sem=self.recv.at[k, lane],
                device_id=(dev,), device_id_type=pl.DeviceIdType.MESH)

        def rows(start, size):
            return pl.ds(pl.multiple_of(start, 64), size)

        row1 = at.c * 256 + d1 * 128
        row2 = row1 + d2 * 64
        if s == 0:
            return [make(self.grads.at[k, rows((1 - at.c) * 256, 256)], self.r0.at[k], 0, at.core_peer)]
        if s == 1:
            return [make(self.grads.at[k, rows(at.c * 256 + (1 - d1) * 128, 128)], self.r1.at[k], 1, p1)]
        if s == 2:
            return [make(self.grads.at[k, rows(row1 + (1 - d2) * 64, 64)], self.r2.at[k], 2, p2)]
        if s == 3:
            cols = [pl.ds(pl.multiple_of(((at.z + 1 + j) % 4) * 128, 128), 128) for j in range(3)]
            return [make(self.grads.at[k, rows(row2, 64), cols[j]], self.r3.at[k, j], 3 + j, at.z_peer(j)) for j in range(3)]
        if s == 4:
            part = self.out.at[k, rows(row2, 64), pl.ds(pl.multiple_of(at.z * 128, 128), 128)]
            return [make(part, part, 6 + j, at.z_peer(j)) for j in range(3)]
        if s == 5:
            part = self.out.at[k, rows(row2, 64)]
            return [make(part, part, 9, p2)]
        if s == 6:
            part = self.out.at[k, rows(row1, 128)]
            return [make(part, part, 10, p1)]
        part = self.out.at[k, rows(at.c * 256, 256)]
        return [make(part, part, 11, at.core_peer)]

    def start(self, s, k):
        for copy in self.copies(s, k):
            copy.start()

    def stage(self, s, k):
        at = self.at
        d1, d2, _, _ = self.spot(k)
        for copy in self.copies(s, k):
            copy.wait_recv()
        row1 = at.c * 256 + d1 * 128
        row2 = row1 + d2 * 64
        if s < 3:
            start, size, landed = ((at.c * 256, 256, self.r0), (row1, 128, self.r1), (row2, 64, self.r2))[s]

            @pl.loop(0, size // 64)
            def _(i):
                mine = (k, pl.ds(pl.multiple_of(start + i * 64, 64), 64))
                theirs = landed[k, pl.ds(pl.multiple_of(i * 64, 64), 64)]
                self.grads[mine] = (self.grads[mine].astype(F32) + theirs.astype(F32)).astype(BF16)
        elif s == 3:
            spot = (k, pl.ds(pl.multiple_of(row2, 64), 64), pl.ds(pl.multiple_of(at.z * 128, 128), 128))
            total = self.grads[spot].astype(F32)
            for j in range(3):
                total = total + self.r3[k, j].astype(F32)
            self.out[spot] = total.astype(BF16)
        if s < 7:
            self.start(s + 1, k)

    def drain(self, k):
        for s in range(8):
            for copy in self.copies(s, k):
                copy.wait_send()


ORDER = (
        (),
        (),
        (),
        (),
        (0, 1),
        (16, 17),
        (32,),
        (),
        (),
        (),
        (),
        (),
        (),
        (),
        (33,),
        (2,),
        (48, 3),
        (4, 5),
        (19, 6, 18),
        (8, 20),
        (49, 34, 7, 21),
        (64, 35),
        (22, 9, 65, 36, 10),
        (37, 23, 80, 50, 24, 81, 12, 38, 51, 11, 25, 52, 26, 39, 53, 97, 40, 66, 96, 68, 67, 54, 27, 55, 41, 42, 112,
     69, 28, 113, 82, 70, 83, 56, 43, 44, 85, 84, 57, 71, 98, 58, 100, 86, 72, 59, 87, 99, 114, 60, 101, 73, 74, 88,
     116, 115, 102, 75, 89, 76, 90, 117, 103, 104, 91, 105, 92, 119, 106, 121, 120, 107, 118, 108, 122, 123, 124),
)


class Progress:
    def __init__(self, red, stores):
        self.red, self.stores, self.point = red, stores, 0

    def ready(self, k):
        self.red.start(0, k)

    def poll(self):
        for code in ORDER[self.point]:
            self.red.stage(code // 16, code % 16)
            if code // 16 == 7:
                self.stores[code % 16].start()
        self.point += 1


def rows_of(i, tile=TILE):
    return pl.ds(pl.multiple_of(i * tile, tile), tile)


def step_kernel(grid_h, mesh_t, edge_t, send_t, src_row, dst_row, w_grid_in_h, w_mesh_in, w_edge_in, w_edge_up_h,
                w_mesh_up_h, w_grid_up_h, w_second_h, vectors, d_mesh_out_h, d_grid_out_h,
                mesh_out_h, grid_out_h, d_grid_h, sums_h,
                grid_t, w_grid_in, w_edge_up, w_mesh_up, w_grid_up, w_second, d_mesh_out, d_grid_out,
                mesh_out, grid_out, d_grid_t, sums, load_sem, store_sem,
                grads, r0, r1, r2, r3, red_send, red_recv, a2a_send, a2a_recv,
                hid0, dsl0, nrm0, inv0, hid1, dsl1, nrm1, inv1, hid2, dsl2, nrm2, inv2, hid3, dsl3, nrm3, inv3,
                hid_s, dlin_s, dpre_s, dlin3, dpre3, dpre4,
                pick_send, pick_src, pick_dst, grid_lat, mesh_lat, cat, edge_new, agg, d_agg, d_edge,
                outgoing, incoming, d_incoming, d_outgoing, d_grid_lat, d_node, d_slot, misc):
    at = Place()
    n_dev = 32
    moves = [(grid_h, grid_t), (w_grid_in_h, w_grid_in), (w_second_h.at[0], w_second.at[0]), (w_grid_up_h, w_grid_up),
             (w_second_h.at[5], w_second.at[5]), (d_grid_out_h, d_grid_out), (w_second_h.at[1], w_second.at[1]),
             (w_second_h.at[2], w_second.at[2]), (w_edge_up_h, w_edge_up), (w_second_h.at[3], w_second.at[3]),
             (w_mesh_up_h, w_mesh_up), (w_second_h.at[4], w_second.at[4]), (d_mesh_out_h, d_mesh_out)]
    loads = [pltpu.make_async_copy(src, dst, load_sem.at[i]) for i, (src, dst) in enumerate(moves)]
    for copy in loads:
        copy.start()
    stores = [pltpu.make_async_copy(sums.at[k], sums_h.at[k], store_sem.at[k]) for k in range(NCHUNK)]
    stores += [pltpu.make_async_copy(src, dst, store_sem.at[NCHUNK + i]) for i, (src, dst) in enumerate(
        [(mesh_out, mesh_out_h), (grid_out, grid_out_h), (d_grid_t, d_grid_h)])]

    def loaded(first, last):
        for copy in loads[first:last]:
            copy.wait()

    barrier = pltpu.get_barrier_semaphore()

    @pl.loop(1, n_dev)
    def _(r):
        pl.semaphore_signal(barrier, inc=1, device_id=((at.p + r) % n_dev,), device_id_type=pl.DeviceIdType.MESH)

    red = Reducer(at, grads, sums, r0, r1, r2, r3, red_send, red_recv)
    prog = Progress(red, stores)

    def vec(k, j):
        return vectors[k, pl.ds(j, 1), :]

    def tail(k, pre, rows, hid):
        pre = pre + vec(k, 0)
        sig = jax.nn.sigmoid(pre)
        act = pre * sig
        hid_bf = act.astype(BF16)
        hid[rows, :] = hid_bf
        out_lin = matmul(hid_bf, w_second[k]) + vec(k, 1)
        centered = out_lin - jnp.mean(out_lin, axis=-1, keepdims=True)
        inv = lax.rsqrt(jnp.mean(centered * centered, axis=-1, keepdims=True) + LN_EPS)
        normed = centered * inv
        return normed * vec(k, 2) + vec(k, 3), sig + act * (1.0 - sig), normed, inv

    def tail_saved(k, pre, rows, saves):
        hid, dsl, nrm, inv_ref = saves
        out, slope, normed, inv = tail(k, pre, rows, hid)
        dsl[rows, :] = slope
        nrm[rows, :] = normed
        inv_ref[rows, :] = inv
        return out

    def tail_back(k, d_out, slope, normed, inv, rows, dlin, dpre):
        d_normed = d_out * vec(k, 2)
        d_lin = inv * (d_normed - jnp.mean(d_normed, axis=-1, keepdims=True)
                       - normed * jnp.mean(d_normed * normed, axis=-1, keepdims=True))
        d_lin_bf = d_lin.astype(BF16)
        dlin[rows, :] = d_lin_bf
        d_pre = contract_cols(d_lin_bf, w_second[k]) * slope
        d_pre_bf = d_pre.astype(BF16)
        dpre[rows, :] = d_pre_bf
        for j, term in enumerate((d_pre, d_lin, d_out * normed, d_out)):
            spot = pl.ds(481 + 4 * k + j, 1)
            misc[spot, :] = misc[spot, :] + jnp.sum(term, axis=0, keepdims=True)
        return d_pre_bf

    def tail_back_saved(k, d_out, rows, saves, dlin, dpre):
        _, dsl, nrm, inv_ref = saves
        return tail_back(k, d_out, dsl[rows, :], nrm[rows, :], inv_ref[rows, :], rows, dlin, dpre)

    def weight_grad(k, lhs, rhs, n_rows, first=0):
        @pl.loop(0, LATENT // TILE)
        def _(i):
            cols = pl.ds(pl.multiple_of(first + i * TILE, TILE), TILE)
            part = contract_rows(lhs[pl.ds(0, n_rows), cols], rhs[pl.ds(0, n_rows), :])
            grads[k, rows_of(i), :] = part.astype(BF16)

    def exchange(src, dst, lane, start):
        def copy(r):
            to = (at.p + r) % n_dev
            return pltpu.make_async_remote_copy(
                src_ref=src.at[pl.ds(pl.multiple_of(to * 16, 16), 16)], dst_ref=dst.at[pl.ds(pl.multiple_of(at.p * 16, 16), 16)],
                send_sem=a2a_send.at[lane, r], recv_sem=a2a_recv.at[lane, r],
                device_id=(to,), device_id_type=pl.DeviceIdType.MESH)

        if start:
            @pl.loop(1, n_dev)
            def _(r):
                copy(r).start()

            mine = pl.ds(pl.multiple_of(at.p * 16, 16), 16)
            dst[mine, :] = src[mine, :]
        else:
            @pl.loop(1, n_dev)
            def _(r):
                copy(r).wait()

    saves0 = (hid0, dsl0, nrm0, inv0)
    saves1 = (hid1, dsl1, nrm1, inv1)
    saves2 = (hid2, dsl2, nrm2, inv2)
    saves3 = (hid3, dsl3, nrm3, inv3)
    misc[pl.ds(472, 40), :] = jnp.zeros((40, LATENT), F32)

    def tiles(n):
        def run(body):
            prog.poll()

            @pl.loop(0, n)
            def _(i):
                body(i, rows_of(i))
        return run

    slots = send_t[...]
    spread = jnp.where(lax.broadcasted_iota(jnp.int32, (32, 512), 0) == lax.broadcasted_iota(jnp.int32, (32, 512), 1) // 16,
                       1.0, 0.0).astype(BF16)
    slots = (matmul((slots // 32).astype(F32).astype(BF16), spread) * 32.0
             + matmul((slots % 32).astype(F32).astype(BF16), spread))
    own = lax.broadcasted_iota(jnp.int32, (16, 512), 0) == lax.broadcasted_iota(jnp.int32, (16, 512), 1) % 16
    send_row = jnp.sum(jnp.where(own, slots, 0.0), axis=0, keepdims=True)

    def pick(row, i):
        ids = lax.broadcasted_iota(jnp.int32, (TILE, row.shape[1]), 0) + i * TILE
        return jnp.where(ids == row, 1.0, 0.0).astype(BF16)

    send_ids = send_row.astype(jnp.int32)
    for i in range(2):
        pick_send[rows_of(i), :] = pick(send_ids, i)

    loaded(0, 3)

    @pl.loop(0, 2)
    def _(i):
        rows = rows_of(i)
        out = tail_saved(0, contract_rows(grid_t[:, rows], w_grid_in[...]), rows, saves0)
        grid_lat[rows, :] = out.astype(BF16)

    @pl.loop(0, 2)
    def _(i):
        rows = rows_of(i)
        outgoing[rows, :] = contract_rows(pick_send[:, rows], grid_lat[...]).astype(BF16)

    pl.semaphore_wait(barrier, n_dev - 1)
    exchange(outgoing, incoming, 0, True)
    loaded(3, 6)

    @tiles(2)
    def _(i, rows):
        lat = grid_lat[rows, :]
        upd, slope, normed, inv = tail(5, matmul(lat, w_grid_up[...]), rows, hid_s)
        grid_out[rows, :] = (lat.astype(F32) + upd).astype(BF16)
        d_top = d_grid_out[rows, :].astype(F32)
        d_pre = tail_back(5, d_top, slope, normed, inv, rows, dlin_s, dpre_s)
        d_grid_lat[rows, :] = d_top + contract_cols(d_pre, w_grid_up[...])

    def grad(k, *args, **kwargs):
        prog.poll()
        weight_grad(k, *args, **kwargs)
        prog.ready(k)

    stores[NCHUNK + 1].start()
    loaded(6, 13)
    grad(0, grid_lat, dpre_s, 512)
    grad(1, hid_s, dlin_s, 512)

    @tiles(2)
    def _(i, rows):
        out = tail_saved(1, contract_rows(mesh_t[:, rows], w_mesh_in[...]), rows, saves1)
        mesh_lat[rows, :] = out.astype(BF16)
        pick_src[rows, :] = pick(src_row[...].reshape(1, 768), i)
        pick_dst[rows, :] = pick(dst_row[...].reshape(1, 768), i)

    @tiles(3)
    def _(i, rows):
        out = tail_saved(2, contract_rows(edge_t[:, rows], w_edge_in[...]), rows, saves2)
        cat[rows, pl.ds(0, 512)] = out.astype(BF16)
        cat[rows, pl.ds(1024, 512)] = contract_rows(pick_dst[:, rows], mesh_lat[...]).astype(BF16)

    prog.poll()
    exchange(outgoing, incoming, 0, False)

    @pl.loop(0, 3)
    def _(i):
        rows = rows_of(i)
        cat[rows, pl.ds(512, 512)] = contract_rows(pick_src[:, rows], incoming[...]).astype(BF16)
        upd = tail_saved(3, matmul(cat[rows, :], w_edge_up[...]), rows, saves3)
        edge_new[rows, :] = (cat[rows, pl.ds(0, 512)].astype(F32) + upd).astype(BF16)

    @tiles(2)
    def _(i, rows):
        lat = mesh_lat[rows, :]
        agg_bf = matmul(pick_dst[rows, :], edge_new[...]).astype(BF16)
        agg[rows, :] = agg_bf
        pre = matmul(lat, w_mesh_up[pl.ds(0, 512), :]) + matmul(agg_bf, w_mesh_up[pl.ds(512, 512), :])
        upd, slope, normed, inv = tail(4, pre, rows, hid_s)
        mesh_out[rows, :] = (lat.astype(F32) + upd).astype(BF16)
        d_pre = tail_back(4, d_mesh_out[rows, :].astype(F32), slope, normed, inv, rows, dlin_s, dpre4)
        d_agg[rows, :] = contract_cols(d_pre, w_mesh_up[pl.ds(512, 512), :]).astype(BF16)

    @tiles(3)
    def _(i, rows):
        d_out = contract_rows(pick_dst[:, rows], d_agg[...])
        d_edge[rows, :] = d_out.astype(BF16)
        tail_back_saved(3, d_out, rows, saves3, dlin3, dpre3)

    @tiles(2)
    def _(i, rows):
        slot = matmul(pick_src[rows, :], dpre3[...]).astype(BF16)
        d_incoming[rows, :] = contract_cols(slot, w_edge_up[pl.ds(512, 512), :]).astype(BF16)

    exchange(d_incoming, d_outgoing, 1, True)
    stores[NCHUNK].start()
    grad(2, mesh_lat, dpre4, 512)
    grad(3, agg, dpre4, 512)
    grad(4, hid_s, dlin_s, 512)
    for part in range(3):
        grad(5 + part, cat, dpre3, 768, first=512 * part)
    grad(8, hid3, dlin3, 768)

    @tiles(3)
    def _(i, rows):
        d_out = d_edge[rows, :].astype(F32) + contract_cols(dpre3[rows, :], w_edge_up[pl.ds(0, 512), :])
        tail_back_saved(2, d_out, rows, saves2, dlin_s, dpre_s)

    misc[pl.ds(477, 4), :] = matmul(edge_t[...], dpre_s[...])
    grad(9, hid2, dlin_s, 768)

    @tiles(2)
    def _(i, rows):
        node = matmul(pick_dst[rows, :], dpre3[...]).astype(BF16)
        d_out = (d_mesh_out[rows, :].astype(F32) + contract_cols(dpre4[rows, :], w_mesh_up[pl.ds(0, 512), :])
                 + contract_cols(node, w_edge_up[pl.ds(1024, 512), :]))
        tail_back_saved(1, d_out, rows, saves1, dlin_s, dpre_s)

    misc[pl.ds(474, 3), :] = matmul(mesh_t[...], dpre_s[pl.ds(0, 512), :])
    grad(10, hid1, dlin_s, 512)
    prog.poll()
    exchange(d_incoming, d_outgoing, 1, False)

    @pl.loop(0, 2)
    def _(i):
        rows = rows_of(i)
        d_out = d_grid_lat[rows, :] + matmul(pick_send[rows, :], d_outgoing[...])
        d_pre = tail_back_saved(0, d_out, rows, saves0, dlin_s, dpre_s)
        d_grid_t[:, rows] = contract_cols(w_grid_in[...], d_pre)

    stores[NCHUNK + 2].start()
    grad(12, hid0, dlin_s, 512)
    prog.poll()
    misc[pl.ds(0, 474), :] = matmul(grid_t[...], dpre_s[pl.ds(0, 512), :])
    grads[11] = misc[...].astype(BF16)
    prog.ready(11)
    prog.poll()

    @pl.loop(0, NCHUNK)
    def _(k):
        red.drain(k)

    for copy in stores:
        copy.wait()


def fused_step(*args):
    def f32(*shape):
        return pltpu.VMEM(shape, F32)

    def bf16(*shape):
        return pltpu.VMEM(shape, BF16)

    def saves(n):
        return [bf16(n, 512), f32(n, 512), f32(n, 512), f32(n, 1)]

    scratch = [
        bf16(474, 512), bf16(474, 512), bf16(1536, 512), bf16(1024, 512), bf16(512, 512), bf16(6, 512, 512), bf16(512, 512),
        bf16(512, 512), bf16(512, 512), bf16(512, 512), f32(474, 512), bf16(NCHUNK, 512, 512),
        pltpu.SemaphoreType.DMA((13,)), pltpu.SemaphoreType.DMA((NCHUNK + 3,)),
        bf16(NCHUNK, 512, 512), bf16(NCHUNK, 256, 512), bf16(NCHUNK, 128, 512), bf16(NCHUNK, 64, 512), bf16(NCHUNK, 3, 64, 128),
        pltpu.SemaphoreType.DMA((NCHUNK, 12)), pltpu.SemaphoreType.DMA((NCHUNK, 12)),
        pltpu.SemaphoreType.DMA((2, 32)), pltpu.SemaphoreType.DMA((2, 32)),
        *saves(512), *saves(512), *saves(768), *saves(768),
        bf16(768, 512), bf16(768, 512), bf16(768, 512), bf16(768, 512), bf16(768, 512), bf16(512, 512),
        bf16(512, 512), bf16(512, 768), bf16(512, 768), bf16(512, 512), bf16(512, 512), bf16(768, 1536), bf16(768, 512),
        bf16(512, 512), bf16(512, 512), bf16(768, 512),
        bf16(512, 512), bf16(512, 512), bf16(512, 512), bf16(512, 512), f32(512, 512), bf16(8, 512), bf16(8, 512), f32(512, 512),
    ]
    return pl.pallas_call(
        step_kernel,
        out_shape=[jax.ShapeDtypeStruct((512, 512), BF16), jax.ShapeDtypeStruct((512, 512), BF16),
                   jax.ShapeDtypeStruct((474, 512), F32), jax.ShapeDtypeStruct((NCHUNK, 512, 512), BF16)],
        in_specs=[pl.BlockSpec(memory_space=pltpu.HBM if i in (0, 6, 9, 10, 11, 12, 14, 15) else pltpu.VMEM)
                  for i in range(len(args))],
        out_specs=[pl.BlockSpec(memory_space=pltpu.HBM)] * 4,
        scratch_shapes=scratch,
        compiler_params=pltpu.CompilerParams(collective_id=0, has_side_effects=True, vmem_limit_bytes=67043328),
    )(*args)


HOME = {0: (2, 0), 1: (3, 5), 2: (1, 0), 3: (1, 1), 4: (3, 4), 5: (0, 0), 6: (0, 1), 7: (0, 2), 8: (3, 3), 9: (3, 2), 10: (3, 1), 12: (3, 0)}


def spread_kernel(mesh_in, grid_in, d_grid_in, sums, mesh_out, grid_out, d_grid_out, edge_up, mesh_up, grid_up, second,
                  w_grid, w_mesh, w_edge, vecs, mesh_buf, grid_buf, d_grid_buf, sum_buf, wide, sem_in, sem_out):
    loads = [pltpu.make_async_copy(sums.at[k], sum_buf.at[k], sem_in.at[k]) for k in range(NCHUNK)]
    through = [(mesh_in, mesh_buf, mesh_out), (grid_in, grid_buf, grid_out), (d_grid_in, d_grid_buf, d_grid_out)]
    heads = [pltpu.make_async_copy(a, b, sem_in.at[NCHUNK + i]) for i, (a, b, _) in enumerate(through)]
    tails = [pltpu.make_async_copy(b, c, sem_out.at[NCHUNK + i]) for i, (_, b, c) in enumerate(through)]
    loads[11].start()
    for k in range(NCHUNK):
        if k != 11:
            loads[k].start()
    for copy in heads:
        copy.start()
    outs = (edge_up, mesh_up, grid_up, second)
    stores = []
    loads[11].wait()
    misc = sum_buf[11].astype(F32)
    w_grid[...] = misc[:474]
    w_mesh[...] = misc[474:477]
    w_edge[...] = misc[477:481]
    for k in range(6):
        vecs[k] = misc[481 + 4 * k:485 + 4 * k]
    for k, (out, part) in HOME.items():
        loads[k].wait()

        @pl.loop(0, 8)
        def _(i):
            rows = rows_of(i, 64)
            wide[k, rows, :] = sum_buf[k, rows, :].astype(F32)

        home = outs[out].at[part] if out == 3 else outs[out].at[pl.ds(part * 512, 512)]
        stores.append(pltpu.make_async_copy(wide.at[k], home, sem_out.at[k]))
        stores[-1].start()
    for head, tail in zip(heads, tails):
        head.wait()
        tail.start()
    for copy in stores + tails:
        copy.wait()


def spread_out(*parts):
    def out(dtype, *shape):
        return jax.ShapeDtypeStruct(shape, dtype)

    anywhere = pl.BlockSpec(memory_space=pltpu.HBM)
    here = pl.BlockSpec(memory_space=pltpu.VMEM)
    mesh_out, grid_out, d_grid, edge_up, mesh_up, grid_up, second, w_grid, w_mesh, w_edge, vecs = pl.pallas_call(
        spread_kernel,
        out_shape=[out(BF16, 512, 512), out(BF16, 512, 512), out(F32, 474, 512), out(F32, 1536, 512), out(F32, 1024, 512),
                   out(F32, 512, 512), out(F32, 6, 512, 512), out(F32, 474, 512), out(F32, 3, 512), out(F32, 4, 512),
                   out(F32, 6, 4, 512)],
        in_specs=[anywhere] * 4,
        out_specs=[anywhere] * 7 + [here] * 4,
        scratch_shapes=[pltpu.VMEM((512, 512), BF16), pltpu.VMEM((512, 512), BF16), pltpu.VMEM((474, 512), F32),
                        pltpu.VMEM((NCHUNK, 512, 512), BF16), pltpu.VMEM((NCHUNK, 512, 512), F32),
                        pltpu.SemaphoreType.DMA((NCHUNK + 3,)), pltpu.SemaphoreType.DMA((NCHUNK + 3,))],
        compiler_params=pltpu.CompilerParams(vmem_limit_bytes=67043328),
    )(*parts)
    return mesh_out, grid_out, d_grid, w_grid, w_mesh, w_edge, edge_up, mesh_up, grid_up, second, vecs


def solution(mesh):
    row_spec = P(AXIS_NAME, None)
    edge_spec = P(AXIS_NAME)
    rep_spec = P()
    in_specs = (row_spec, row_spec, row_spec, row_spec, edge_spec, edge_spec) + (rep_spec,) * 8 + (row_spec, row_spec)
    out_specs = (row_spec, row_spec, row_spec) + (rep_spec,) * 8

    def local_step(grid_in, mesh_static, edge_static, send_rows, edge_src, edge_dst, *rest):
        parts = fused_step(grid_in.T, mesh_static.T, edge_static.T, send_rows.T,
                           edge_src, edge_dst, *rest)
        mesh_out, grid_out, d_grid_t, *sums = spread_out(*parts)
        return (mesh_out, grid_out, d_grid_t.T) + tuple(sums)

    return jax.shard_map(local_step, mesh=mesh, in_specs=in_specs, out_specs=out_specs, check_vma=False)
```

```python
import jax
import jax.numpy as jnp
from jax import lax
from jax.experimental import pallas as pl
from jax.experimental.pallas import tpu as pltpu
from jax.sharding import PartitionSpec as P

LN_EPS = 1e-5
AXIS_NAME = 'gp'
NCHUNK = 13
TILE = 256
LATENT = 512
F32 = jnp.float32
BF16 = jnp.bfloat16


def matmul(lhs, rhs):
    return jnp.dot(lhs, rhs, preferred_element_type=jnp.float32)


def contract_rows(lhs, rhs):
    return lax.dot_general(lhs, rhs, (((0,), (0,)), ((), ())), preferred_element_type=jnp.float32)


def contract_cols(lhs, rhs):
    return lax.dot_general(lhs, rhs, (((1,), (1,)), ((), ())), preferred_element_type=jnp.float32)


class Place:
    def __init__(self):
        self.p = lax.axis_index(AXIS_NAME)
        self.bit = {axis: (self.p // 2 ** i) % 2 for i, axis in enumerate('cxyuv')}
        self.peer = {axis: self.p + 2 ** i * (1 - 2 * self.bit[axis]) for i, axis in enumerate('cxyuv')}


class Reducer:
    def __init__(self, at, grads, land, out, send, recv):
        self.at, self.grads, self.land, self.out, self.send, self.recv = at, grads, land, out, send, recv

    def axes(self, k):
        return 'c' + AXES[k]

    def regions(self, k):
        row, rows, col, cols = 0, 512, 0, 512
        kept, sent = [], []
        for axis in self.axes(k):
            bit = self.at.bit[axis]
            if axis in 'cxy':
                rows //= 2
                sent.append((row + (1 - bit) * rows, rows, col, cols))
                row = row + bit * rows
            else:
                cols //= 2
                sent.append((row, rows, col + (1 - bit) * cols, cols))
                col = col + bit * cols
            kept.append((row, rows, col, cols))
        return kept, sent

    def index(self, k, region, step=0, tile=None):
        row, rows, col, cols = region
        lanes = pl.ds(0, 512) if cols == 512 else pl.ds(pl.multiple_of(col, 128), cols)
        return k, pl.ds(pl.multiple_of(row + step, 64), tile or rows), lanes

    def copy(self, s, k):
        kept, sent = self.regions(k)
        turn = s if s < 5 else 9 - s
        if s < 5:
            src, dst = self.grads.at[self.index(k, sent[s])], self.land.at[self.index(k, kept[s])]
        else:
            src = dst = self.out.at[self.index(k, kept[turn])]
        return pltpu.make_async_remote_copy(
            src_ref=src, dst_ref=dst, send_sem=self.send.at[k, s], recv_sem=self.recv.at[k, s],
            device_id=(self.at.peer[self.axes(k)[turn]],), device_id_type=pl.DeviceIdType.MESH)

    def start(self, s, k):
        self.copy(s, k).start()

    def stage(self, s, k):
        self.copy(s, k).wait_recv()
        if s < 5:
            kept, sent = self.regions(k)
            into = self.out if s == 4 else self.grads

            def add(step):
                mine = self.index(k, kept[s], step, 64)
                theirs = self.land[self.index(k, sent[s], step, 64)]
                into[mine] = (self.grads[mine].astype(F32) + theirs.astype(F32)).astype(BF16)

            if kept[s][1] == 64:
                add(0)
            else:
                @pl.loop(0, kept[s][1] // 64)
                def _(i):
                    add(i * 64)
        if s < 9:
            self.start(s + 1, k)

    def drain(self):
        for k in range(NCHUNK):
            for s in range(10):
                self.copy(s, k).wait_send()


AXES = ('xvuy', 'yuvx', 'uyxv', 'yxuv', 'xyuv', 'yxuv', 'xyuv', 'uvxy', 'xyuv', 'yxuv', 'xyuv', 'yxuv', 'xyuv')
ORDER = (
        (),
        (),
        (),
        (),
        (0, 1),
        (16, 17),
        (),
        (32, 33),
        (48,),
        (),
        (),
        (),
        (),
        (),
        (64,),
        (),
        (49,),
        (4, 2, 3, 5, 65, 80),
        (6,),
        (81, 7, 19, 20, 8, 96, 18),
        (22,),
        (97, 21, 9, 36, 34, 23),
        (10,),
        (35, 24, 38, 52, 12, 113, 37, 50, 51, 54, 112, 68, 40, 53, 26, 66, 11, 67, 28, 39, 129, 70, 84, 69, 42, 56, 25,
     83, 86, 82, 100, 55, 27, 85, 72, 99, 41, 128, 58, 98, 44, 101, 71, 145, 43, 116, 102, 57, 88, 60, 144, 115, 74, 59,
     114, 118, 73, 87, 104, 76, 132, 90, 117, 120, 131, 75, 89, 92, 134, 130, 106, 103, 147, 105, 136, 122, 91, 108,
     121, 119, 133, 107, 124, 150, 138, 123, 146, 137, 135, 140, 153, 139, 156, 149, 148, 151, 154, 152, 155),
)


class Progress:
    def __init__(self, red, stores):
        self.red, self.stores, self.point = red, stores, 0

    def ready(self, k):
        self.red.start(0, k)

    def poll(self):
        for code in ORDER[self.point]:
            self.red.stage(code // 16, code % 16)
            if code // 16 == 9:
                self.stores[code % 16].start()
        self.point += 1


def rows_of(i, tile=TILE):
    return pl.ds(pl.multiple_of(i * tile, tile), tile)


def step_kernel(grid_h, mesh_t, edge_t, send_t, src_row, dst_row, w_grid_in_h, w_mesh_in, w_edge_in, w_edge_up_h,
                w_mesh_up_h, w_grid_up_h, w_second_h, vectors, d_mesh_out_h, d_grid_out_h,
                mesh_out_h, grid_out_h, d_grid_h, sums_h,
                grid_t, w_grid_in, w_edge_up, w_mesh_up, w_grid_up, w_second, d_mesh_out, d_grid_out,
                mesh_out, grid_out, d_grid_t, sums, load_sem, store_sem,
                grads, land, red_send, red_recv, a2a_send, a2a_recv,
                hid0, dsl0, nrm0, inv0, hid1, dsl1, nrm1, inv1, hid2, dsl2, nrm2, inv2, hid3, dsl3, nrm3, inv3,
                hid_s, dlin_s, dpre_s, dlin3, dpre3, dpre4,
                pick_send, pick_src, pick_dst, grid_lat, mesh_lat, cat, edge_new, agg, d_agg, d_edge,
                outgoing, incoming, d_incoming, d_outgoing, d_grid_lat, d_node, d_slot, misc):
    at = Place()
    n_dev = 32
    moves = [(grid_h, grid_t), (w_grid_in_h, w_grid_in), (w_second_h.at[0], w_second.at[0]), (w_grid_up_h, w_grid_up),
             (w_second_h.at[5], w_second.at[5]), (d_grid_out_h, d_grid_out), (w_second_h.at[1], w_second.at[1]),
             (w_second_h.at[2], w_second.at[2]), (w_edge_up_h, w_edge_up), (w_second_h.at[3], w_second.at[3]),
             (w_mesh_up_h, w_mesh_up), (w_second_h.at[4], w_second.at[4]), (d_mesh_out_h, d_mesh_out)]
    loads = [pltpu.make_async_copy(src, dst, load_sem.at[i]) for i, (src, dst) in enumerate(moves)]
    for copy in loads:
        copy.start()
    stores = [pltpu.make_async_copy(sums.at[k], sums_h.at[k], store_sem.at[k]) for k in range(NCHUNK)]
    stores += [pltpu.make_async_copy(src, dst, store_sem.at[NCHUNK + i]) for i, (src, dst) in enumerate(
        [(mesh_out, mesh_out_h), (grid_out, grid_out_h), (d_grid_t, d_grid_h)])]

    def loaded(first, last):
        for copy in loads[first:last]:
            copy.wait()

    barrier = pltpu.get_barrier_semaphore()

    @pl.loop(1, n_dev)
    def _(r):
        pl.semaphore_signal(barrier, inc=1, device_id=((at.p + r) % n_dev,), device_id_type=pl.DeviceIdType.MESH)

    red = Reducer(at, grads, land, sums, red_send, red_recv)
    prog = Progress(red, stores)

    def vec(k, j):
        return vectors[k, pl.ds(j, 1), :]

    def tail(k, pre, rows, hid):
        pre = pre + vec(k, 0)
        sig = jax.nn.sigmoid(pre)
        act = pre * sig
        hid_bf = act.astype(BF16)
        hid[rows, :] = hid_bf
        out_lin = matmul(hid_bf, w_second[k]) + vec(k, 1)
        centered = out_lin - jnp.mean(out_lin, axis=-1, keepdims=True)
        inv = lax.rsqrt(jnp.mean(centered * centered, axis=-1, keepdims=True) + LN_EPS)
        normed = centered * inv
        return normed * vec(k, 2) + vec(k, 3), sig + act * (1.0 - sig), normed, inv

    def tail_saved(k, pre, rows, saves):
        hid, dsl, nrm, inv_ref = saves
        out, slope, normed, inv = tail(k, pre, rows, hid)
        dsl[rows, :] = slope
        nrm[rows, :] = normed
        inv_ref[rows, :] = inv
        return out

    def tail_back(k, d_out, slope, normed, inv, rows, dlin, dpre):
        d_normed = d_out * vec(k, 2)
        d_lin = inv * (d_normed - jnp.mean(d_normed, axis=-1, keepdims=True)
                       - normed * jnp.mean(d_normed * normed, axis=-1, keepdims=True))
        d_lin_bf = d_lin.astype(BF16)
        dlin[rows, :] = d_lin_bf
        d_pre = contract_cols(d_lin_bf, w_second[k]) * slope
        d_pre_bf = d_pre.astype(BF16)
        dpre[rows, :] = d_pre_bf
        for j, term in enumerate((d_pre, d_lin, d_out * normed, d_out)):
            spot = pl.ds(481 + 4 * k + j, 1)
            misc[spot, :] = misc[spot, :] + jnp.sum(term, axis=0, keepdims=True)
        return d_pre_bf

    def tail_back_saved(k, d_out, rows, saves, dlin, dpre):
        _, dsl, nrm, inv_ref = saves
        return tail_back(k, d_out, dsl[rows, :], nrm[rows, :], inv_ref[rows, :], rows, dlin, dpre)

    def weight_grad(k, lhs, rhs, n_rows, first=0):
        @pl.loop(0, LATENT // TILE)
        def _(i):
            cols = pl.ds(pl.multiple_of(first + i * TILE, TILE), TILE)
            part = contract_rows(lhs[pl.ds(0, n_rows), cols], rhs[pl.ds(0, n_rows), :])
            grads[k, rows_of(i), :] = part.astype(BF16)

    def exchange(src, dst, lane, start):
        def copy(r):
            to = (at.p + r) % n_dev
            return pltpu.make_async_remote_copy(
                src_ref=src.at[pl.ds(pl.multiple_of(to * 16, 16), 16)], dst_ref=dst.at[pl.ds(pl.multiple_of(at.p * 16, 16), 16)],
                send_sem=a2a_send.at[lane, r], recv_sem=a2a_recv.at[lane, r],
                device_id=(to,), device_id_type=pl.DeviceIdType.MESH)

        if start:
            @pl.loop(1, n_dev)
            def _(r):
                copy(r).start()

            mine = pl.ds(pl.multiple_of(at.p * 16, 16), 16)
            dst[mine, :] = src[mine, :]
        else:
            @pl.loop(1, n_dev)
            def _(r):
                copy(r).wait()

    saves0 = (hid0, dsl0, nrm0, inv0)
    saves1 = (hid1, dsl1, nrm1, inv1)
    saves2 = (hid2, dsl2, nrm2, inv2)
    saves3 = (hid3, dsl3, nrm3, inv3)
    misc[pl.ds(472, 40), :] = jnp.zeros((40, LATENT), F32)

    def tiles(n):
        def run(body):
            prog.poll()

            @pl.loop(0, n)
            def _(i):
                body(i, rows_of(i))
        return run

    slots = send_t[...]
    spread = jnp.where(lax.broadcasted_iota(jnp.int32, (32, 512), 0) == lax.broadcasted_iota(jnp.int32, (32, 512), 1) // 16,
                       1.0, 0.0).astype(BF16)
    slots = (matmul((slots // 32).astype(F32).astype(BF16), spread) * 32.0
             + matmul((slots % 32).astype(F32).astype(BF16), spread))
    own = lax.broadcasted_iota(jnp.int32, (16, 512), 0) == lax.broadcasted_iota(jnp.int32, (16, 512), 1) % 16
    send_row = jnp.sum(jnp.where(own, slots, 0.0), axis=0, keepdims=True)

    def pick(row, i):
        ids = lax.broadcasted_iota(jnp.int32, (TILE, row.shape[1]), 0) + i * TILE
        return jnp.where(ids == row, 1.0, 0.0).astype(BF16)

    send_ids = send_row.astype(jnp.int32)
    for i in range(2):
        pick_send[rows_of(i), :] = pick(send_ids, i)

    loaded(0, 3)

    @pl.loop(0, 2)
    def _(i):
        rows = rows_of(i)
        out = tail_saved(0, contract_rows(grid_t[:, rows], w_grid_in[...]), rows, saves0)
        grid_lat[rows, :] = out.astype(BF16)

    @pl.loop(0, 2)
    def _(i):
        rows = rows_of(i)
        outgoing[rows, :] = contract_rows(pick_send[:, rows], grid_lat[...]).astype(BF16)

    pl.semaphore_wait(barrier, n_dev - 1)
    exchange(outgoing, incoming, 0, True)
    loaded(3, 6)

    @tiles(2)
    def _(i, rows):
        lat = grid_lat[rows, :]
        upd, slope, normed, inv = tail(5, matmul(lat, w_grid_up[...]), rows, hid_s)
        grid_out[rows, :] = (lat.astype(F32) + upd).astype(BF16)
        d_top = d_grid_out[rows, :].astype(F32)
        d_pre = tail_back(5, d_top, slope, normed, inv, rows, dlin_s, dpre_s)
        d_grid_lat[rows, :] = d_top + contract_cols(d_pre, w_grid_up[...])

    def grad(k, *args, **kwargs):
        prog.poll()
        weight_grad(k, *args, **kwargs)
        prog.ready(k)

    stores[NCHUNK + 1].start()
    loaded(6, 13)
    grad(0, grid_lat, dpre_s, 512)
    grad(1, hid_s, dlin_s, 512)

    @tiles(2)
    def _(i, rows):
        out = tail_saved(1, contract_rows(mesh_t[:, rows], w_mesh_in[...]), rows, saves1)
        mesh_lat[rows, :] = out.astype(BF16)
        pick_src[rows, :] = pick(src_row[...].reshape(1, 768), i)
        pick_dst[rows, :] = pick(dst_row[...].reshape(1, 768), i)

    @tiles(3)
    def _(i, rows):
        out = tail_saved(2, contract_rows(edge_t[:, rows], w_edge_in[...]), rows, saves2)
        cat[rows, pl.ds(0, 512)] = out.astype(BF16)
        recv = contract_rows(pick_dst[:, rows], mesh_lat[...]).astype(BF16)
        cat[rows, pl.ds(1024, 512)] = recv
        nrm3[rows, :] = matmul(out.astype(BF16), w_edge_up[pl.ds(0, 512), :]) + matmul(recv, w_edge_up[pl.ds(1024, 512), :])

    prog.poll()
    exchange(outgoing, incoming, 0, False)

    @pl.loop(0, 3)
    def _(i):
        rows = rows_of(i)
        sender = contract_rows(pick_src[:, rows], incoming[...]).astype(BF16)
        cat[rows, pl.ds(512, 512)] = sender
        upd = tail_saved(3, nrm3[rows, :] + matmul(sender, w_edge_up[pl.ds(512, 512), :]), rows, saves3)
        edge_new[rows, :] = (cat[rows, pl.ds(0, 512)].astype(F32) + upd).astype(BF16)

    @tiles(2)
    def _(i, rows):
        lat = mesh_lat[rows, :]
        agg_bf = matmul(pick_dst[rows, :], edge_new[...]).astype(BF16)
        agg[rows, :] = agg_bf
        pre = matmul(lat, w_mesh_up[pl.ds(0, 512), :]) + matmul(agg_bf, w_mesh_up[pl.ds(512, 512), :])
        upd, slope, normed, inv = tail(4, pre, rows, hid_s)
        mesh_out[rows, :] = (lat.astype(F32) + upd).astype(BF16)
        d_pre = tail_back(4, d_mesh_out[rows, :].astype(F32), slope, normed, inv, rows, dlin_s, dpre4)
        d_agg[rows, :] = contract_cols(d_pre, w_mesh_up[pl.ds(512, 512), :]).astype(BF16)

    @tiles(3)
    def _(i, rows):
        d_out = contract_rows(pick_dst[:, rows], d_agg[...])
        d_edge[rows, :] = d_out.astype(BF16)
        tail_back_saved(3, d_out, rows, saves3, dlin3, dpre3)

    @tiles(2)
    def _(i, rows):
        slot = matmul(pick_src[rows, :], dpre3[...]).astype(BF16)
        d_incoming[rows, :] = contract_cols(slot, w_edge_up[pl.ds(512, 512), :]).astype(BF16)

    exchange(d_incoming, d_outgoing, 1, True)
    stores[NCHUNK].start()
    grad(2, mesh_lat, dpre4, 512)
    grad(3, agg, dpre4, 512)
    grad(4, hid_s, dlin_s, 512)
    for part in range(3):
        grad(5 + part, cat, dpre3, 768, first=512 * part)
    grad(8, hid3, dlin3, 768)

    @tiles(3)
    def _(i, rows):
        d_out = d_edge[rows, :].astype(F32) + contract_cols(dpre3[rows, :], w_edge_up[pl.ds(0, 512), :])
        tail_back_saved(2, d_out, rows, saves2, dlin_s, dpre_s)

    misc[pl.ds(477, 4), :] = matmul(edge_t[...], dpre_s[...])
    grad(9, hid2, dlin_s, 768)

    @tiles(2)
    def _(i, rows):
        node = matmul(pick_dst[rows, :], dpre3[...]).astype(BF16)
        d_out = (d_mesh_out[rows, :].astype(F32) + contract_cols(dpre4[rows, :], w_mesh_up[pl.ds(0, 512), :])
                 + contract_cols(node, w_edge_up[pl.ds(1024, 512), :]))
        tail_back_saved(1, d_out, rows, saves1, dlin_s, dpre_s)

    misc[pl.ds(474, 3), :] = matmul(mesh_t[...], dpre_s[pl.ds(0, 512), :])
    grad(10, hid1, dlin_s, 512)
    prog.poll()
    exchange(d_incoming, d_outgoing, 1, False)

    @pl.loop(0, 2)
    def _(i):
        rows = rows_of(i)
        d_out = d_grid_lat[rows, :] + matmul(pick_send[rows, :], d_outgoing[...])
        d_pre = tail_back_saved(0, d_out, rows, saves0, dlin_s, dpre_s)
        d_grid_t[:, rows] = contract_cols(w_grid_in[...], d_pre)

    stores[NCHUNK + 2].start()
    grad(12, hid0, dlin_s, 512)
    prog.poll()
    misc[pl.ds(0, 474), :] = matmul(grid_t[...], dpre_s[pl.ds(0, 512), :])
    grads[11] = misc[...].astype(BF16)
    prog.ready(11)
    prog.poll()

    red.drain()

    for copy in stores:
        copy.wait()


def fused_step(*args):
    def f32(*shape):
        return pltpu.VMEM(shape, F32)

    def bf16(*shape):
        return pltpu.VMEM(shape, BF16)

    def saves(n):
        return [bf16(n, 512), f32(n, 512), f32(n, 512), f32(n, 1)]

    scratch = [
        bf16(474, 512), bf16(474, 512), bf16(1536, 512), bf16(1024, 512), bf16(512, 512), bf16(6, 512, 512), bf16(512, 512),
        bf16(512, 512), bf16(512, 512), bf16(512, 512), f32(474, 512), bf16(NCHUNK, 512, 512),
        pltpu.SemaphoreType.DMA((13,)), pltpu.SemaphoreType.DMA((NCHUNK + 3,)),
        bf16(NCHUNK, 512, 512), bf16(NCHUNK, 512, 512), pltpu.SemaphoreType.DMA((NCHUNK, 10)), pltpu.SemaphoreType.DMA((NCHUNK, 10)),
        pltpu.SemaphoreType.DMA((2, 32)), pltpu.SemaphoreType.DMA((2, 32)),
        *saves(512), *saves(512), *saves(768), *saves(768),
        bf16(768, 512), bf16(768, 512), bf16(768, 512), bf16(768, 512), bf16(768, 512), bf16(512, 512),
        bf16(512, 512), bf16(512, 768), bf16(512, 768), bf16(512, 512), bf16(512, 512), bf16(768, 1536), bf16(768, 512),
        bf16(512, 512), bf16(512, 512), bf16(768, 512),
        bf16(512, 512), bf16(512, 512), bf16(512, 512), bf16(512, 512), f32(512, 512), bf16(8, 512), bf16(8, 512), f32(512, 512),
    ]
    return pl.pallas_call(
        step_kernel,
        out_shape=[jax.ShapeDtypeStruct((512, 512), BF16), jax.ShapeDtypeStruct((512, 512), BF16),
                   jax.ShapeDtypeStruct((474, 512), F32), jax.ShapeDtypeStruct((NCHUNK, 512, 512), BF16)],
        in_specs=[pl.BlockSpec(memory_space=pltpu.HBM if i in (0, 6, 9, 10, 11, 12, 14, 15) else pltpu.VMEM)
                  for i in range(len(args))],
        out_specs=[pl.BlockSpec(memory_space=pltpu.HBM)] * 4,
        scratch_shapes=scratch,
        compiler_params=pltpu.CompilerParams(collective_id=0, has_side_effects=True, vmem_limit_bytes=67043328),
    )(*args)


HOME = {0: (2, 0), 1: (3, 5), 2: (1, 0), 3: (1, 1), 4: (3, 4), 5: (0, 0), 6: (0, 1), 7: (0, 2), 8: (3, 3), 9: (3, 2), 10: (3, 1), 12: (3, 0)}


def spread_kernel(mesh_in, grid_in, d_grid_in, sums, mesh_out, grid_out, d_grid_out, edge_up, mesh_up, grid_up, second,
                  w_grid, w_mesh, w_edge, vecs, mesh_buf, grid_buf, d_grid_buf, sum_buf, wide, sem_in, sem_out):
    loads = [pltpu.make_async_copy(sums.at[k], sum_buf.at[k], sem_in.at[k]) for k in range(NCHUNK)]
    through = [(mesh_in, mesh_buf, mesh_out), (grid_in, grid_buf, grid_out), (d_grid_in, d_grid_buf, d_grid_out)]
    heads = [pltpu.make_async_copy(a, b, sem_in.at[NCHUNK + i]) for i, (a, b, _) in enumerate(through)]
    tails = [pltpu.make_async_copy(b, c, sem_out.at[NCHUNK + i]) for i, (_, b, c) in enumerate(through)]
    loads[11].start()
    for k in range(NCHUNK):
        if k != 11:
            loads[k].start()
    for copy in heads:
        copy.start()
    outs = (edge_up, mesh_up, grid_up, second)
    stores = []
    loads[11].wait()
    misc = sum_buf[11].astype(F32)
    w_grid[...] = misc[:474]
    w_mesh[...] = misc[474:477]
    w_edge[...] = misc[477:481]
    for k in range(6):
        vecs[k] = misc[481 + 4 * k:485 + 4 * k]
    for k, (out, part) in HOME.items():
        loads[k].wait()

        @pl.loop(0, 8)
        def _(i):
            rows = rows_of(i, 64)
            wide[k, rows, :] = sum_buf[k, rows, :].astype(F32)

        home = outs[out].at[part] if out == 3 else outs[out].at[pl.ds(part * 512, 512)]
        stores.append(pltpu.make_async_copy(wide.at[k], home, sem_out.at[k]))
        stores[-1].start()
    for head, tail in zip(heads, tails):
        head.wait()
        tail.start()
    for copy in stores + tails:
        copy.wait()


def spread_out(*parts):
    def out(dtype, *shape):
        return jax.ShapeDtypeStruct(shape, dtype)

    anywhere = pl.BlockSpec(memory_space=pltpu.HBM)
    here = pl.BlockSpec(memory_space=pltpu.VMEM)
    mesh_out, grid_out, d_grid, edge_up, mesh_up, grid_up, second, w_grid, w_mesh, w_edge, vecs = pl.pallas_call(
        spread_kernel,
        out_shape=[out(BF16, 512, 512), out(BF16, 512, 512), out(F32, 474, 512), out(F32, 1536, 512), out(F32, 1024, 512),
                   out(F32, 512, 512), out(F32, 6, 512, 512), out(F32, 474, 512), out(F32, 3, 512), out(F32, 4, 512),
                   out(F32, 6, 4, 512)],
        in_specs=[anywhere] * 4,
        out_specs=[anywhere] * 7 + [here] * 4,
        scratch_shapes=[pltpu.VMEM((512, 512), BF16), pltpu.VMEM((512, 512), BF16), pltpu.VMEM((474, 512), F32),
                        pltpu.VMEM((NCHUNK, 512, 512), BF16), pltpu.VMEM((NCHUNK, 512, 512), F32),
                        pltpu.SemaphoreType.DMA((NCHUNK + 3,)), pltpu.SemaphoreType.DMA((NCHUNK + 3,))],
        compiler_params=pltpu.CompilerParams(vmem_limit_bytes=67043328),
    )(*parts)
    return mesh_out, grid_out, d_grid, w_grid, w_mesh, w_edge, edge_up, mesh_up, grid_up, second, vecs


def solution(mesh):
    row_spec = P(AXIS_NAME, None)
    edge_spec = P(AXIS_NAME)
    rep_spec = P()
    in_specs = (row_spec, row_spec, row_spec, row_spec, edge_spec, edge_spec) + (rep_spec,) * 8 + (row_spec, row_spec)
    out_specs = (row_spec, row_spec, row_spec) + (rep_spec,) * 8

    def local_step(grid_in, mesh_static, edge_static, send_rows, edge_src, edge_dst, *rest):
        parts = fused_step(grid_in.T, mesh_static.T, edge_static.T, send_rows.T,
                           edge_src, edge_dst, *rest)
        mesh_out, grid_out, d_grid_t, *sums = spread_out(*parts)
        return (mesh_out, grid_out, d_grid_t.T) + tuple(sums)

    return jax.shard_map(local_step, mesh=mesh, in_specs=in_specs, out_specs=out_specs, check_vma=False)
```

```python
import jax
import jax.numpy as jnp
from jax import lax
from jax.experimental import pallas as pl
from jax.experimental.pallas import tpu as pltpu
from jax.sharding import PartitionSpec as P

LN_EPS = 1e-5
AXIS_NAME = 'gp'
NCHUNK = 13
TILE = 256
LATENT = 512
F32 = jnp.float32
BF16 = jnp.bfloat16


def matmul(lhs, rhs):
    return jnp.dot(lhs, rhs, preferred_element_type=jnp.float32)


def contract_rows(lhs, rhs):
    return lax.dot_general(lhs, rhs, (((0,), (0,)), ((), ())), preferred_element_type=jnp.float32)


def contract_cols(lhs, rhs):
    return lax.dot_general(lhs, rhs, (((1,), (1,)), ((), ())), preferred_element_type=jnp.float32)


class Place:
    def __init__(self):
        self.p = lax.axis_index(AXIS_NAME)
        self.c = self.p % 2
        self.x = (self.p // 2) % 2
        self.y = (self.p // 4) % 2
        self.z = self.p // 8
        self.core_peer = self.p + 1 - 2 * self.c
        self.x_peer = self.p + 2 - 4 * self.x
        self.y_peer = self.p + 4 - 8 * self.y

    def z_peer(self, j):
        return self.p % 8 + ((self.z + 1 + j) % 4) * 8


class Reducer:
    def __init__(self, at, grads, out, r0, r1, r2, r3, send, recv):
        self.at = at
        self.grads, self.out = grads, out
        self.r0, self.r1, self.r2, self.r3 = r0, r1, r2, r3
        self.send, self.recv = send, recv

    def spot(self, k):
        at = self.at
        odd = k % 2
        d1 = at.x * (1 - odd) + at.y * odd
        d2 = at.y * (1 - odd) + at.x * odd
        p1 = at.x_peer * (1 - odd) + at.y_peer * odd
        p2 = at.y_peer * (1 - odd) + at.x_peer * odd
        return d1, d2, p1, p2

    def copies(self, s, k):
        at = self.at
        d1, d2, p1, p2 = self.spot(k)

        def make(src, dst, lane, dev):
            return pltpu.make_async_remote_copy(
                src_ref=src, dst_ref=dst, send_sem=self.send.at[k, lane], recv_sem=self.recv.at[k, lane],
                device_id=(dev,), device_id_type=pl.DeviceIdType.MESH)

        def rows(start, size):
            return pl.ds(pl.multiple_of(start, 64), size)

        row1 = at.c * 256 + d1 * 128
        row2 = row1 + d2 * 64
        if s == 0:
            return [make(self.grads.at[k, rows((1 - at.c) * 256, 256)], self.r0.at[k], 0, at.core_peer)]
        if s == 1:
            return [make(self.grads.at[k, rows(at.c * 256 + (1 - d1) * 128, 128)], self.r1.at[k], 1, p1)]
        if s == 2:
            return [make(self.grads.at[k, rows(row1 + (1 - d2) * 64, 64)], self.r2.at[k], 2, p2)]
        if s == 3:
            cols = [pl.ds(pl.multiple_of(((at.z + 1 + j) % 4) * 128, 128), 128) for j in range(3)]
            return [make(self.grads.at[k, rows(row2, 64), cols[j]], self.r3.at[k, j], 3 + j, at.z_peer(j)) for j in range(3)]
        if s == 4:
            part = self.out.at[k, rows(row2, 64), pl.ds(pl.multiple_of(at.z * 128, 128), 128)]
            return [make(part, part, 6 + j, at.z_peer(j)) for j in range(3)]
        if s == 5:
            part = self.out.at[k, rows(row2, 64)]
            return [make(part, part, 9, p2)]
        if s == 6:
            part = self.out.at[k, rows(row1, 128)]
            return [make(part, part, 10, p1)]
        part = self.out.at[k, rows(at.c * 256, 256)]
        return [make(part, part, 11, at.core_peer)]

    def start(self, s, k):
        for copy in self.copies(s, k):
            copy.start()

    def stage(self, s, k):
        at = self.at
        d1, d2, _, _ = self.spot(k)
        for copy in self.copies(s, k):
            copy.wait_recv()
        row1 = at.c * 256 + d1 * 128
        row2 = row1 + d2 * 64
        if s < 3:
            start, size, landed = ((at.c * 256, 256, self.r0), (row1, 128, self.r1), (row2, 64, self.r2))[s]

            @pl.loop(0, size // 64)
            def _(i):
                mine = (k, pl.ds(pl.multiple_of(start + i * 64, 64), 64))
                theirs = landed[k, pl.ds(pl.multiple_of(i * 64, 64), 64)]
                self.grads[mine] = (self.grads[mine].astype(F32) + theirs.astype(F32)).astype(BF16)
        elif s == 3:
            spot = (k, pl.ds(pl.multiple_of(row2, 64), 64), pl.ds(pl.multiple_of(at.z * 128, 128), 128))
            total = self.grads[spot].astype(F32)
            for j in range(3):
                total = total + self.r3[k, j].astype(F32)
            self.out[spot] = total.astype(BF16)
        if s < 7:
            self.start(s + 1, k)

    def drain(self, k):
        for s in range(8):
            for copy in self.copies(s, k):
                copy.wait_send()


ORDER = (
        (),
        (),
        (),
        (),
        (0, 1),
        (16, 17),
        (32,),
        (),
        (),
        (),
        (),
        (33,),
        (48,),
        (),
        (),
        (2,),
        (3,),
        (4, 5),
        (18, 6),
        (7, 21),
        (20, 19, 34, 8, 49),
        (64, 37, 22, 35),
        (23,),
        (36, 65, 9, 10, 80, 53, 24, 38, 11, 52, 51, 50, 26, 40, 25, 39, 81, 54, 12, 69, 67, 68, 42, 56, 66, 27, 41, 28,
     84, 83, 70, 55, 82, 44, 43, 97, 96, 85, 113, 72, 57, 71, 99, 86, 58, 100, 87, 98, 59, 73, 60, 101, 88, 74, 89, 75,
     102, 103, 90, 76, 104, 91, 105, 116, 118, 92, 115, 106, 120, 107, 121, 117, 108, 122, 112, 123, 119, 114, 124),
)


class Progress:
    def __init__(self, red, stores):
        self.red, self.stores, self.point = red, stores, 0

    def ready(self, k):
        self.red.start(0, k)

    def poll(self):
        for code in ORDER[self.point]:
            self.red.stage(code // 16, code % 16)
            if code // 16 == 7:
                self.stores[code % 16].start()
        self.point += 1


def rows_of(i, tile=TILE):
    return pl.ds(pl.multiple_of(i * tile, tile), tile)


def step_kernel(grid_h, mesh_t, edge_t, send_t, src_row, dst_row, w_grid_in_h, w_mesh_in, w_edge_in, w_edge_up_h,
                w_mesh_up_h, w_grid_up_h, w_second_h, vectors, d_mesh_out_h, d_grid_out_h,
                mesh_out_h, grid_out_h, d_grid_h, sums_h,
                grid_t, w_grid_in, w_edge_up, w_mesh_up, w_grid_up, w_second, d_mesh_out, d_grid_out,
                mesh_out, grid_out, d_grid_t, sums, load_sem, store_sem,
                grads, r0, r1, r2, r3, red_send, red_recv, a2a_send, a2a_recv,
                hid0, dsl0, nrm0, inv0, hid1, dsl1, nrm1, inv1, hid2, dsl2, nrm2, inv2, hid3, dsl3, nrm3, inv3,
                hid_s, dlin_s, dpre_s, dlin3, dpre3, dpre4,
                pick_send, pick_src, pick_dst, grid_lat, mesh_lat, cat, edge_new, agg, d_agg, d_edge,
                outgoing, incoming, d_incoming, d_outgoing, d_grid_lat, d_node, d_slot, misc):
    at = Place()
    n_dev = 32
    moves = [(grid_h, grid_t), (w_grid_in_h, w_grid_in), (w_second_h.at[0], w_second.at[0]), (w_grid_up_h, w_grid_up),
             (w_second_h.at[5], w_second.at[5]), (d_grid_out_h, d_grid_out), (w_second_h.at[1], w_second.at[1]),
             (w_second_h.at[2], w_second.at[2]), (w_edge_up_h, w_edge_up), (w_second_h.at[3], w_second.at[3]),
             (w_mesh_up_h, w_mesh_up), (w_second_h.at[4], w_second.at[4]), (d_mesh_out_h, d_mesh_out)]
    loads = [pltpu.make_async_copy(src, dst, load_sem.at[i]) for i, (src, dst) in enumerate(moves)]
    for copy in loads:
        copy.start()
    stores = [pltpu.make_async_copy(sums.at[k], sums_h.at[k], store_sem.at[k]) for k in range(NCHUNK)]
    stores += [pltpu.make_async_copy(src, dst, store_sem.at[NCHUNK + i]) for i, (src, dst) in enumerate(
        [(mesh_out, mesh_out_h), (grid_out, grid_out_h), (d_grid_t, d_grid_h)])]

    def loaded(first, last):
        for copy in loads[first:last]:
            copy.wait()

    barrier = pltpu.get_barrier_semaphore()

    @pl.loop(1, n_dev)
    def _(r):
        pl.semaphore_signal(barrier, inc=1, device_id=((at.p + r) % n_dev,), device_id_type=pl.DeviceIdType.MESH)

    red = Reducer(at, grads, sums, r0, r1, r2, r3, red_send, red_recv)
    prog = Progress(red, stores)

    def vec(k, j):
        return vectors[k, pl.ds(j, 1), :]

    def tail(k, pre, rows, hid):
        pre = pre + vec(k, 0)
        sig = jax.nn.sigmoid(pre)
        act = pre * sig
        hid_bf = act.astype(BF16)
        hid[rows, :] = hid_bf
        out_lin = matmul(hid_bf, w_second[k]) + vec(k, 1)
        centered = out_lin - jnp.mean(out_lin, axis=-1, keepdims=True)
        inv = lax.rsqrt(jnp.mean(centered * centered, axis=-1, keepdims=True) + LN_EPS)
        normed = centered * inv
        return normed * vec(k, 2) + vec(k, 3), sig + act * (1.0 - sig), normed, inv

    def tail_saved(k, pre, rows, saves):
        hid, dsl, nrm, inv_ref = saves
        out, slope, normed, inv = tail(k, pre, rows, hid)
        dsl[rows, :] = slope
        nrm[rows, :] = normed
        inv_ref[rows, :] = inv
        return out

    def tail_back(k, d_out, slope, normed, inv, rows, dlin, dpre):
        d_normed = d_out * vec(k, 2)
        d_lin = inv * (d_normed - jnp.mean(d_normed, axis=-1, keepdims=True)
                       - normed * jnp.mean(d_normed * normed, axis=-1, keepdims=True))
        d_lin_bf = d_lin.astype(BF16)
        dlin[rows, :] = d_lin_bf
        d_pre = contract_cols(d_lin_bf, w_second[k]) * slope
        d_pre_bf = d_pre.astype(BF16)
        dpre[rows, :] = d_pre_bf
        for j, term in enumerate((d_pre, d_lin, d_out * normed, d_out)):
            spot = pl.ds(481 + 4 * k + j, 1)
            misc[spot, :] = misc[spot, :] + jnp.sum(term, axis=0, keepdims=True)
        return d_pre_bf

    def tail_back_saved(k, d_out, rows, saves, dlin, dpre):
        _, dsl, nrm, inv_ref = saves
        return tail_back(k, d_out, dsl[rows, :], nrm[rows, :], inv_ref[rows, :], rows, dlin, dpre)

    def weight_grad(k, lhs, rhs, n_rows, first=0):
        @pl.loop(0, LATENT // TILE)
        def _(i):
            cols = pl.ds(pl.multiple_of(first + i * TILE, TILE), TILE)
            part = contract_rows(lhs[pl.ds(0, n_rows), cols], rhs[pl.ds(0, n_rows), :])
            grads[k, rows_of(i), :] = part.astype(BF16)

    def exchange(src, dst, lane, start):
        low = at.p % 8

        def copy(turn, j):
            peer_z = (at.z % 2 + turn % 2) % 2 + 2 * ((at.z // 2 + turn // 2) % 2)
            to = peer_z * 8 + (low + j) % 8
            return pltpu.make_async_remote_copy(
                src_ref=src.at[pl.ds(pl.multiple_of(to * 16, 16), 16)], dst_ref=dst.at[pl.ds(pl.multiple_of(at.p * 16, 16), 16)],
                send_sem=a2a_send.at[lane, turn * 8 + j], recv_sem=a2a_recv.at[lane, turn * 8 + j],
                device_id=(to,), device_id_type=pl.DeviceIdType.MESH)

        for turn in (3, 2, 1, 0):
            @pl.loop(0 if turn else 1, 8)
            def _(j):
                if start:
                    copy(turn, j).start()
                else:
                    copy(turn, j).wait()

        if start:
            mine = pl.ds(pl.multiple_of(at.p * 16, 16), 16)
            dst[mine, :] = src[mine, :]

    saves0 = (hid0, dsl0, nrm0, inv0)
    saves1 = (hid1, dsl1, nrm1, inv1)
    saves2 = (hid2, dsl2, nrm2, inv2)
    saves3 = (hid3, dsl3, nrm3, inv3)
    misc[pl.ds(472, 40), :] = jnp.zeros((40, LATENT), F32)

    def tiles(n):
        def run(body):
            prog.poll()

            @pl.loop(0, n)
            def _(i):
                body(i, rows_of(i))
        return run

    slots = send_t[...]
    spread = jnp.where(lax.broadcasted_iota(jnp.int32, (32, 512), 0) == lax.broadcasted_iota(jnp.int32, (32, 512), 1) // 16,
                       1.0, 0.0).astype(BF16)
    slots = (matmul((slots // 32).astype(F32).astype(BF16), spread) * 32.0
             + matmul((slots % 32).astype(F32).astype(BF16), spread))
    own = lax.broadcasted_iota(jnp.int32, (16, 512), 0) == lax.broadcasted_iota(jnp.int32, (16, 512), 1) % 16
    send_row = jnp.sum(jnp.where(own, slots, 0.0), axis=0, keepdims=True)

    def pick(row, i):
        ids = lax.broadcasted_iota(jnp.int32, (TILE, row.shape[1]), 0) + i * TILE
        return jnp.where(ids == row, 1.0, 0.0).astype(BF16)

    send_ids = send_row.astype(jnp.int32)
    for i in range(2):
        pick_send[rows_of(i), :] = pick(send_ids, i)

    loaded(0, 3)

    @pl.loop(0, 2)
    def _(i):
        rows = rows_of(i)
        out = tail_saved(0, contract_rows(grid_t[:, rows], w_grid_in[...]), rows, saves0)
        grid_lat[rows, :] = out.astype(BF16)

    @pl.loop(0, 2)
    def _(i):
        rows = rows_of(i)
        outgoing[rows, :] = contract_rows(pick_send[:, rows], grid_lat[...]).astype(BF16)

    pl.semaphore_wait(barrier, n_dev - 1)
    exchange(outgoing, incoming, 0, True)
    loaded(3, 6)

    @tiles(2)
    def _(i, rows):
        lat = grid_lat[rows, :]
        upd, slope, normed, inv = tail(5, matmul(lat, w_grid_up[...]), rows, hid_s)
        grid_out[rows, :] = (lat.astype(F32) + upd).astype(BF16)
        d_top = d_grid_out[rows, :].astype(F32)
        d_pre = tail_back(5, d_top, slope, normed, inv, rows, dlin_s, dpre_s)
        d_grid_lat[rows, :] = d_top + contract_cols(d_pre, w_grid_up[...])

    def grad(k, *args, **kwargs):
        prog.poll()
        weight_grad(k, *args, **kwargs)
        prog.ready(k)

    stores[NCHUNK + 1].start()
    loaded(6, 13)
    grad(0, grid_lat, dpre_s, 512)
    grad(1, hid_s, dlin_s, 512)

    @tiles(2)
    def _(i, rows):
        out = tail_saved(1, contract_rows(mesh_t[:, rows], w_mesh_in[...]), rows, saves1)
        mesh_lat[rows, :] = out.astype(BF16)
        pick_src[rows, :] = pick(src_row[...].reshape(1, 768), i)
        pick_dst[rows, :] = pick(dst_row[...].reshape(1, 768), i)

    @tiles(3)
    def _(i, rows):
        out = tail_saved(2, contract_rows(edge_t[:, rows], w_edge_in[...]), rows, saves2)
        cat[rows, pl.ds(0, 512)] = out.astype(BF16)
        recv = contract_rows(pick_dst[:, rows], mesh_lat[...]).astype(BF16)
        cat[rows, pl.ds(1024, 512)] = recv
        nrm3[rows, :] = matmul(out.astype(BF16), w_edge_up[pl.ds(0, 512), :]) + matmul(recv, w_edge_up[pl.ds(1024, 512), :])

    prog.poll()
    exchange(outgoing, incoming, 0, False)

    @pl.loop(0, 3)
    def _(i):
        rows = rows_of(i)
        sender = contract_rows(pick_src[:, rows], incoming[...]).astype(BF16)
        cat[rows, pl.ds(512, 512)] = sender
        upd = tail_saved(3, nrm3[rows, :] + matmul(sender, w_edge_up[pl.ds(512, 512), :]), rows, saves3)
        edge_new[rows, :] = (cat[rows, pl.ds(0, 512)].astype(F32) + upd).astype(BF16)

    @tiles(2)
    def _(i, rows):
        lat = mesh_lat[rows, :]
        agg_bf = matmul(pick_dst[rows, :], edge_new[...]).astype(BF16)
        agg[rows, :] = agg_bf
        pre = matmul(lat, w_mesh_up[pl.ds(0, 512), :]) + matmul(agg_bf, w_mesh_up[pl.ds(512, 512), :])
        upd, slope, normed, inv = tail(4, pre, rows, hid_s)
        mesh_out[rows, :] = (lat.astype(F32) + upd).astype(BF16)
        d_pre = tail_back(4, d_mesh_out[rows, :].astype(F32), slope, normed, inv, rows, dlin_s, dpre4)
        d_agg[rows, :] = contract_cols(d_pre, w_mesh_up[pl.ds(512, 512), :]).astype(BF16)

    @tiles(3)
    def _(i, rows):
        d_out = contract_rows(pick_dst[:, rows], d_agg[...])
        d_edge[rows, :] = d_out.astype(BF16)
        tail_back_saved(3, d_out, rows, saves3, dlin3, dpre3)

    @tiles(2)
    def _(i, rows):
        slot = matmul(pick_src[rows, :], dpre3[...]).astype(BF16)
        d_incoming[rows, :] = contract_cols(slot, w_edge_up[pl.ds(512, 512), :]).astype(BF16)

    exchange(d_incoming, d_outgoing, 1, True)
    stores[NCHUNK].start()
    grad(2, mesh_lat, dpre4, 512)
    grad(3, agg, dpre4, 512)
    grad(4, hid_s, dlin_s, 512)
    for part in range(3):
        grad(5 + part, cat, dpre3, 768, first=512 * part)
    grad(8, hid3, dlin3, 768)

    @tiles(3)
    def _(i, rows):
        d_out = d_edge[rows, :].astype(F32) + contract_cols(dpre3[rows, :], w_edge_up[pl.ds(0, 512), :])
        tail_back_saved(2, d_out, rows, saves2, dlin_s, dpre_s)

    misc[pl.ds(477, 4), :] = matmul(edge_t[...], dpre_s[...])
    grad(9, hid2, dlin_s, 768)

    @tiles(2)
    def _(i, rows):
        node = matmul(pick_dst[rows, :], dpre3[...]).astype(BF16)
        d_out = (d_mesh_out[rows, :].astype(F32) + contract_cols(dpre4[rows, :], w_mesh_up[pl.ds(0, 512), :])
                 + contract_cols(node, w_edge_up[pl.ds(1024, 512), :]))
        tail_back_saved(1, d_out, rows, saves1, dlin_s, dpre_s)

    misc[pl.ds(474, 3), :] = matmul(mesh_t[...], dpre_s[pl.ds(0, 512), :])
    grad(10, hid1, dlin_s, 512)
    prog.poll()
    exchange(d_incoming, d_outgoing, 1, False)

    @pl.loop(0, 2)
    def _(i):
        rows = rows_of(i)
        d_out = d_grid_lat[rows, :] + matmul(pick_send[rows, :], d_outgoing[...])
        d_pre = tail_back_saved(0, d_out, rows, saves0, dlin_s, dpre_s)
        d_grid_t[:, rows] = contract_cols(w_grid_in[...], d_pre)

    stores[NCHUNK + 2].start()
    grad(12, hid0, dlin_s, 512)
    prog.poll()
    misc[pl.ds(0, 474), :] = matmul(grid_t[...], dpre_s[pl.ds(0, 512), :])
    grads[11] = misc[...].astype(BF16)
    prog.ready(11)
    prog.poll()

    @pl.loop(0, NCHUNK)
    def _(k):
        red.drain(k)

    for copy in stores:
        copy.wait()


def fused_step(*args):
    def f32(*shape):
        return pltpu.VMEM(shape, F32)

    def bf16(*shape):
        return pltpu.VMEM(shape, BF16)

    def saves(n):
        return [bf16(n, 512), f32(n, 512), f32(n, 512), f32(n, 1)]

    scratch = [
        bf16(474, 512), bf16(474, 512), bf16(1536, 512), bf16(1024, 512), bf16(512, 512), bf16(6, 512, 512), bf16(512, 512),
        bf16(512, 512), bf16(512, 512), bf16(512, 512), f32(474, 512), bf16(NCHUNK, 512, 512),
        pltpu.SemaphoreType.DMA((13,)), pltpu.SemaphoreType.DMA((NCHUNK + 3,)),
        bf16(NCHUNK, 512, 512), bf16(NCHUNK, 256, 512), bf16(NCHUNK, 128, 512), bf16(NCHUNK, 64, 512), bf16(NCHUNK, 3, 64, 128),
        pltpu.SemaphoreType.DMA((NCHUNK, 12)), pltpu.SemaphoreType.DMA((NCHUNK, 12)),
        pltpu.SemaphoreType.DMA((2, 32)), pltpu.SemaphoreType.DMA((2, 32)),
        *saves(512), *saves(512), *saves(768), *saves(768),
        bf16(768, 512), bf16(768, 512), bf16(768, 512), bf16(768, 512), bf16(768, 512), bf16(512, 512),
        bf16(512, 512), bf16(512, 768), bf16(512, 768), bf16(512, 512), bf16(512, 512), bf16(768, 1536), bf16(768, 512),
        bf16(512, 512), bf16(512, 512), bf16(768, 512),
        bf16(512, 512), bf16(512, 512), bf16(512, 512), bf16(512, 512), f32(512, 512), bf16(8, 512), bf16(8, 512), f32(512, 512),
    ]
    return pl.pallas_call(
        step_kernel,
        out_shape=[jax.ShapeDtypeStruct((512, 512), BF16), jax.ShapeDtypeStruct((512, 512), BF16),
                   jax.ShapeDtypeStruct((474, 512), F32), jax.ShapeDtypeStruct((NCHUNK, 512, 512), BF16)],
        in_specs=[pl.BlockSpec(memory_space=pltpu.HBM if i in (0, 6, 9, 10, 11, 12, 14, 15) else pltpu.VMEM)
                  for i in range(len(args))],
        out_specs=[pl.BlockSpec(memory_space=pltpu.HBM)] * 4,
        scratch_shapes=scratch,
        compiler_params=pltpu.CompilerParams(collective_id=0, has_side_effects=True, vmem_limit_bytes=67043328),
    )(*args)


HOME = {0: (2, 0), 1: (3, 5), 2: (1, 0), 3: (1, 1), 4: (3, 4), 5: (0, 0), 6: (0, 1), 7: (0, 2), 8: (3, 3), 9: (3, 2), 10: (3, 1), 12: (3, 0)}


def spread_kernel(mesh_in, grid_in, d_grid_in, sums, mesh_out, grid_out, d_grid_out, edge_up, mesh_up, grid_up, second,
                  w_grid, w_mesh, w_edge, vecs, mesh_buf, grid_buf, d_grid_buf, sum_buf, wide, sem_in, sem_out):
    loads = [pltpu.make_async_copy(sums.at[k], sum_buf.at[k], sem_in.at[k]) for k in range(NCHUNK)]
    through = [(mesh_in, mesh_buf, mesh_out), (grid_in, grid_buf, grid_out), (d_grid_in, d_grid_buf, d_grid_out)]
    heads = [pltpu.make_async_copy(a, b, sem_in.at[NCHUNK + i]) for i, (a, b, _) in enumerate(through)]
    tails = [pltpu.make_async_copy(b, c, sem_out.at[NCHUNK + i]) for i, (_, b, c) in enumerate(through)]
    loads[11].start()
    for k in range(NCHUNK):
        if k != 11:
            loads[k].start()
    for copy in heads:
        copy.start()
    outs = (edge_up, mesh_up, grid_up, second)
    stores = []
    loads[11].wait()
    misc = sum_buf[11].astype(F32)
    w_grid[...] = misc[:474]
    w_mesh[...] = misc[474:477]
    w_edge[...] = misc[477:481]
    for k in range(6):
        vecs[k] = misc[481 + 4 * k:485 + 4 * k]
    for k, (out, part) in HOME.items():
        loads[k].wait()

        @pl.loop(0, 8)
        def _(i):
            rows = rows_of(i, 64)
            wide[k, rows, :] = sum_buf[k, rows, :].astype(F32)

        home = outs[out].at[part] if out == 3 else outs[out].at[pl.ds(part * 512, 512)]
        stores.append(pltpu.make_async_copy(wide.at[k], home, sem_out.at[k]))
        stores[-1].start()
    for head, tail in zip(heads, tails):
        head.wait()
        tail.start()
    for copy in stores + tails:
        copy.wait()


def spread_out(*parts):
    def out(dtype, *shape):
        return jax.ShapeDtypeStruct(shape, dtype)

    anywhere = pl.BlockSpec(memory_space=pltpu.HBM)
    here = pl.BlockSpec(memory_space=pltpu.VMEM)
    mesh_out, grid_out, d_grid, edge_up, mesh_up, grid_up, second, w_grid, w_mesh, w_edge, vecs = pl.pallas_call(
        spread_kernel,
        out_shape=[out(BF16, 512, 512), out(BF16, 512, 512), out(F32, 474, 512), out(F32, 1536, 512), out(F32, 1024, 512),
                   out(F32, 512, 512), out(F32, 6, 512, 512), out(F32, 474, 512), out(F32, 3, 512), out(F32, 4, 512),
                   out(F32, 6, 4, 512)],
        in_specs=[anywhere] * 4,
        out_specs=[anywhere] * 7 + [here] * 4,
        scratch_shapes=[pltpu.VMEM((512, 512), BF16), pltpu.VMEM((512, 512), BF16), pltpu.VMEM((474, 512), F32),
                        pltpu.VMEM((NCHUNK, 512, 512), BF16), pltpu.VMEM((NCHUNK, 512, 512), F32),
                        pltpu.SemaphoreType.DMA((NCHUNK + 3,)), pltpu.SemaphoreType.DMA((NCHUNK + 3,))],
        compiler_params=pltpu.CompilerParams(vmem_limit_bytes=67043328),
    )(*parts)
    return mesh_out, grid_out, d_grid, w_grid, w_mesh, w_edge, edge_up, mesh_up, grid_up, second, vecs


def solution(mesh):
    row_spec = P(AXIS_NAME, None)
    edge_spec = P(AXIS_NAME)
    rep_spec = P()
    in_specs = (row_spec, row_spec, row_spec, row_spec, edge_spec, edge_spec) + (rep_spec,) * 8 + (row_spec, row_spec)
    out_specs = (row_spec, row_spec, row_spec) + (rep_spec,) * 8

    def local_step(grid_in, mesh_static, edge_static, send_rows, edge_src, edge_dst, *rest):
        parts = fused_step(grid_in.T, mesh_static.T, edge_static.T, send_rows.T,
                           edge_src, edge_dst, *rest)
        mesh_out, grid_out, d_grid_t, *sums = spread_out(*parts)
        return (mesh_out, grid_out, d_grid_t.T) + tuple(sums)

    return jax.shard_map(local_step, mesh=mesh, in_specs=in_specs, out_specs=out_specs, check_vma=False)
```

```python
import jax
import jax.numpy as jnp
from jax import lax
from jax.experimental import pallas as pl
from jax.experimental.pallas import tpu as pltpu
from jax.sharding import PartitionSpec as P

LN_EPS = 1e-5
AXIS_NAME = 'gp'
NCHUNK = 13
TILE = 256
LATENT = 512
F32 = jnp.float32
BF16 = jnp.bfloat16


def matmul(lhs, rhs):
    return jnp.dot(lhs, rhs, preferred_element_type=jnp.float32)


def contract_rows(lhs, rhs):
    return lax.dot_general(lhs, rhs, (((0,), (0,)), ((), ())), preferred_element_type=jnp.float32)


def contract_cols(lhs, rhs):
    return lax.dot_general(lhs, rhs, (((1,), (1,)), ((), ())), preferred_element_type=jnp.float32)


class Place:
    def __init__(self):
        self.p = lax.axis_index(AXIS_NAME)
        self.c = self.p % 2
        self.x = (self.p // 2) % 2
        self.y = (self.p // 4) % 2
        self.z = self.p // 8
        self.core_peer = self.p + 1 - 2 * self.c
        self.x_peer = self.p + 2 - 4 * self.x
        self.y_peer = self.p + 4 - 8 * self.y

    def z_peer(self, j):
        return self.p % 8 + ((self.z + 1 + j) % 4) * 8


class Reducer:
    def __init__(self, at, grads, out, r0, r1, r2, r3, send, recv):
        self.at = at
        self.grads, self.out = grads, out
        self.r0, self.r1, self.r2, self.r3 = r0, r1, r2, r3
        self.send, self.recv = send, recv

    def spot(self, k):
        at = self.at
        odd = k % 2
        d1 = at.x * (1 - odd) + at.y * odd
        d2 = at.y * (1 - odd) + at.x * odd
        p1 = at.x_peer * (1 - odd) + at.y_peer * odd
        p2 = at.y_peer * (1 - odd) + at.x_peer * odd
        return d1, d2, p1, p2

    def copies(self, s, k):
        at = self.at
        d1, d2, p1, p2 = self.spot(k)

        def make(src, dst, lane, dev):
            return pltpu.make_async_remote_copy(
                src_ref=src, dst_ref=dst, send_sem=self.send.at[k, lane], recv_sem=self.recv.at[k, lane],
                device_id=(dev,), device_id_type=pl.DeviceIdType.MESH)

        def rows(start, size):
            return pl.ds(pl.multiple_of(start, 64), size)

        row1 = at.c * 256 + d1 * 128
        row2 = row1 + d2 * 64
        if s == 0:
            return [make(self.grads.at[k, rows((1 - at.c) * 256, 256)], self.r0.at[k], 0, at.core_peer)]
        if s == 1:
            return [make(self.grads.at[k, rows(at.c * 256 + (1 - d1) * 128, 128)], self.r1.at[k], 1, p1)]
        if s == 2:
            return [make(self.grads.at[k, rows(row1 + (1 - d2) * 64, 64)], self.r2.at[k], 2, p2)]
        if s == 3:
            cols = [pl.ds(pl.multiple_of(((at.z + 1 + j) % 4) * 128, 128), 128) for j in range(3)]
            return [make(self.grads.at[k, rows(row2, 64), cols[j]], self.r3.at[k, j], 3 + j, at.z_peer(j)) for j in range(3)]
        if s == 4:
            part = self.out.at[k, rows(row2, 64), pl.ds(pl.multiple_of(at.z * 128, 128), 128)]
            return [make(part, part, 6 + j, at.z_peer(j)) for j in range(3)]
        if s == 5:
            part = self.out.at[k, rows(row2, 64)]
            return [make(part, part, 9, p2)]
        if s == 6:
            part = self.out.at[k, rows(row1, 128)]
            return [make(part, part, 10, p1)]
        part = self.out.at[k, rows(at.c * 256, 256)]
        return [make(part, part, 11, at.core_peer)]

    def start(self, s, k):
        for copy in self.copies(s, k):
            copy.start()

    def stage(self, s, k):
        at = self.at
        d1, d2, _, _ = self.spot(k)
        for copy in self.copies(s, k):
            copy.wait_recv()
        row1 = at.c * 256 + d1 * 128
        row2 = row1 + d2 * 64
        if s < 3:
            start, size, landed = ((at.c * 256, 256, self.r0), (row1, 128, self.r1), (row2, 64, self.r2))[s]

            @pl.loop(0, size // 64)
            def _(i):
                mine = (k, pl.ds(pl.multiple_of(start + i * 64, 64), 64))
                theirs = landed[k, pl.ds(pl.multiple_of(i * 64, 64), 64)]
                self.grads[mine] = (self.grads[mine].astype(F32) + theirs.astype(F32)).astype(BF16)
        elif s == 3:
            spot = (k, pl.ds(pl.multiple_of(row2, 64), 64), pl.ds(pl.multiple_of(at.z * 128, 128), 128))
            total = self.grads[spot].astype(F32)
            for j in range(3):
                total = total + self.r3[k, j].astype(F32)
            self.out[spot] = total.astype(BF16)
        if s < 7:
            self.start(s + 1, k)

    def drain(self, k):
        for s in range(8):
            for copy in self.copies(s, k):
                copy.wait_send()


ORDER = (
        (),
        (),
        (),
        (),
        (0, 1),
        (16, 17),
        (32,),
        (),
        (),
        (),
        (),
        (),
        (),
        (),
        (33,),
        (2,),
        (48, 3),
        (4, 5),
        (19, 6, 18),
        (8, 20),
        (49, 34, 7, 21),
        (64, 35),
        (22, 9, 65, 36, 10),
        (37, 23, 80, 50, 24, 81, 12, 38, 51, 11, 25, 52, 26, 39, 53, 97, 40, 66, 96, 68, 67, 54, 27, 55, 41, 42, 112,
     69, 28, 113, 82, 70, 83, 56, 43, 44, 85, 84, 57, 71, 98, 58, 100, 86, 72, 59, 87, 99, 114, 60, 101, 73, 74, 88,
     116, 115, 102, 75, 89, 76, 90, 117, 103, 104, 91, 105, 92, 119, 106, 121, 120, 107, 118, 108, 122, 123, 124),
)


class Progress:
    def __init__(self, red, stores):
        self.red, self.stores, self.point = red, stores, 0

    def ready(self, k):
        self.red.start(0, k)

    def poll(self):
        for code in ORDER[self.point]:
            self.red.stage(code // 16, code % 16)
            if code // 16 == 7:
                self.stores[code % 16].start()
        self.point += 1


def rows_of(i, tile=TILE):
    return pl.ds(pl.multiple_of(i * tile, tile), tile)


def step_kernel(grid_h, mesh_t, edge_t, send_t, src_row, dst_row, w_grid_in_h, w_mesh_in, w_edge_in, w_edge_up_h,
                w_mesh_up_h, w_grid_up_h, w_second_h, vectors, d_mesh_out_h, d_grid_out_h,
                mesh_out_h, grid_out_h, d_grid_h, sums_h,
                grid_t, w_grid_in, w_edge_up, w_mesh_up, w_grid_up, w_second, d_mesh_out, d_grid_out,
                mesh_out, grid_out, d_grid_t, sums, load_sem, store_sem,
                grads, r0, r1, r2, r3, red_send, red_recv, a2a_send, a2a_recv,
                hid0, dsl0, nrm0, inv0, hid1, dsl1, nrm1, inv1, hid2, dsl2, nrm2, inv2, hid3, dsl3, nrm3, inv3,
                hid_s, dlin_s, dpre_s, dlin3, dpre3, dpre4,
                pick_send, pick_src, pick_dst, grid_lat, mesh_lat, cat, edge_new, agg, d_agg, d_edge,
                outgoing, incoming, d_incoming, d_outgoing, d_grid_lat, d_node, d_slot, misc):
    at = Place()
    n_dev = 32
    moves = [(grid_h, grid_t), (w_grid_in_h, w_grid_in), (w_second_h.at[0], w_second.at[0]), (w_grid_up_h, w_grid_up),
             (w_second_h.at[5], w_second.at[5]), (d_grid_out_h, d_grid_out), (w_second_h.at[1], w_second.at[1]),
             (w_second_h.at[2], w_second.at[2]), (w_edge_up_h, w_edge_up), (w_second_h.at[3], w_second.at[3]),
             (w_mesh_up_h, w_mesh_up), (w_second_h.at[4], w_second.at[4]), (d_mesh_out_h, d_mesh_out)]
    loads = [pltpu.make_async_copy(src, dst, load_sem.at[i]) for i, (src, dst) in enumerate(moves)]
    for copy in loads:
        copy.start()
    stores = [pltpu.make_async_copy(sums.at[k], sums_h.at[k], store_sem.at[k]) for k in range(NCHUNK)]
    stores += [pltpu.make_async_copy(src, dst, store_sem.at[NCHUNK + i]) for i, (src, dst) in enumerate(
        [(mesh_out, mesh_out_h), (grid_out, grid_out_h), (d_grid_t, d_grid_h)])]

    def loaded(first, last):
        for copy in loads[first:last]:
            copy.wait()

    barrier = pltpu.get_barrier_semaphore()

    @pl.loop(1, n_dev)
    def _(r):
        pl.semaphore_signal(barrier, inc=1, device_id=((at.p + r) % n_dev,), device_id_type=pl.DeviceIdType.MESH)

    red = Reducer(at, grads, sums, r0, r1, r2, r3, red_send, red_recv)
    prog = Progress(red, stores)

    def vec(k, j):
        return vectors[k, pl.ds(j, 1), :]

    def tail(k, pre, rows, hid):
        pre = pre + vec(k, 0)
        sig = jax.nn.sigmoid(pre)
        act = pre * sig
        hid_bf = act.astype(BF16)
        hid[rows, :] = hid_bf
        out_lin = matmul(hid_bf, w_second[k]) + vec(k, 1)
        centered = out_lin - jnp.mean(out_lin, axis=-1, keepdims=True)
        inv = lax.rsqrt(jnp.mean(centered * centered, axis=-1, keepdims=True) + LN_EPS)
        normed = centered * inv
        return normed * vec(k, 2) + vec(k, 3), sig + act * (1.0 - sig), normed, inv

    def tail_saved(k, pre, rows, saves):
        hid, dsl, nrm, inv_ref = saves
        out, slope, normed, inv = tail(k, pre, rows, hid)
        dsl[rows, :] = slope
        nrm[rows, :] = normed
        inv_ref[rows, :] = inv
        return out

    def tail_back(k, d_out, slope, normed, inv, rows, dlin, dpre):
        d_normed = d_out * vec(k, 2)
        d_lin = inv * (d_normed - jnp.mean(d_normed, axis=-1, keepdims=True)
                       - normed * jnp.mean(d_normed * normed, axis=-1, keepdims=True))
        d_lin_bf = d_lin.astype(BF16)
        dlin[rows, :] = d_lin_bf
        d_pre = contract_cols(d_lin_bf, w_second[k]) * slope
        d_pre_bf = d_pre.astype(BF16)
        dpre[rows, :] = d_pre_bf
        for j, term in enumerate((d_pre, d_lin, d_out * normed, d_out)):
            spot = pl.ds(481 + 4 * k + j, 1)
            misc[spot, :] = misc[spot, :] + jnp.sum(term, axis=0, keepdims=True)
        return d_pre_bf

    def tail_back_saved(k, d_out, rows, saves, dlin, dpre):
        _, dsl, nrm, inv_ref = saves
        return tail_back(k, d_out, dsl[rows, :], nrm[rows, :], inv_ref[rows, :], rows, dlin, dpre)

    def weight_grad(k, lhs, rhs, n_rows, first=0):
        @pl.loop(0, LATENT // TILE)
        def _(i):
            cols = pl.ds(pl.multiple_of(first + i * TILE, TILE), TILE)
            part = contract_rows(lhs[pl.ds(0, n_rows), cols], rhs[pl.ds(0, n_rows), :])
            grads[k, rows_of(i), :] = part.astype(BF16)

    def exchange(src, dst, lane, start):
        low = at.p % 8

        def copy(turn, j):
            peer_z = (at.z % 2 + turn % 2) % 2 + 2 * ((at.z // 2 + turn // 2) % 2)
            to = peer_z * 8 + (low + j) % 8
            return pltpu.make_async_remote_copy(
                src_ref=src.at[pl.ds(pl.multiple_of(to * 16, 16), 16)], dst_ref=dst.at[pl.ds(pl.multiple_of(at.p * 16, 16), 16)],
                send_sem=a2a_send.at[lane, turn * 8 + j], recv_sem=a2a_recv.at[lane, turn * 8 + j],
                device_id=(to,), device_id_type=pl.DeviceIdType.MESH)

        for turn in (3, 2, 1, 0):
            @pl.loop(0 if turn else 1, 8)
            def _(j):
                if start:
                    copy(turn, j).start()
                else:
                    copy(turn, j).wait()

        if start:
            mine = pl.ds(pl.multiple_of(at.p * 16, 16), 16)
            dst[mine, :] = src[mine, :]

    saves0 = (hid0, dsl0, nrm0, inv0)
    saves1 = (hid1, dsl1, nrm1, inv1)
    saves2 = (hid2, dsl2, nrm2, inv2)
    saves3 = (hid3, dsl3, nrm3, inv3)
    misc[pl.ds(472, 40), :] = jnp.zeros((40, LATENT), F32)

    def tiles(n):
        def run(body):
            prog.poll()

            @pl.loop(0, n)
            def _(i):
                body(i, rows_of(i))
        return run

    slots = send_t[...]
    spread = jnp.where(lax.broadcasted_iota(jnp.int32, (32, 512), 0) == lax.broadcasted_iota(jnp.int32, (32, 512), 1) // 16,
                       1.0, 0.0).astype(BF16)
    slots = (matmul((slots // 32).astype(F32).astype(BF16), spread) * 32.0
             + matmul((slots % 32).astype(F32).astype(BF16), spread))
    own = lax.broadcasted_iota(jnp.int32, (16, 512), 0) == lax.broadcasted_iota(jnp.int32, (16, 512), 1) % 16
    send_row = jnp.sum(jnp.where(own, slots, 0.0), axis=0, keepdims=True)

    def pick(row, i):
        ids = lax.broadcasted_iota(jnp.int32, (TILE, row.shape[1]), 0) + i * TILE
        return jnp.where(ids == row, 1.0, 0.0).astype(BF16)

    send_ids = send_row.astype(jnp.int32)
    for i in range(2):
        pick_send[rows_of(i), :] = pick(send_ids, i)

    loaded(0, 3)

    @pl.loop(0, 2)
    def _(i):
        rows = rows_of(i)
        out = tail_saved(0, contract_rows(grid_t[:, rows], w_grid_in[...]), rows, saves0)
        grid_lat[rows, :] = out.astype(BF16)

    @pl.loop(0, 2)
    def _(i):
        rows = rows_of(i)
        outgoing[rows, :] = contract_rows(pick_send[:, rows], grid_lat[...]).astype(BF16)

    pl.semaphore_wait(barrier, n_dev - 1)
    exchange(outgoing, incoming, 0, True)
    loaded(3, 6)

    @tiles(2)
    def _(i, rows):
        lat = grid_lat[rows, :]
        upd, slope, normed, inv = tail(5, matmul(lat, w_grid_up[...]), rows, hid_s)
        grid_out[rows, :] = (lat.astype(F32) + upd).astype(BF16)
        d_top = d_grid_out[rows, :].astype(F32)
        d_pre = tail_back(5, d_top, slope, normed, inv, rows, dlin_s, dpre_s)
        d_grid_lat[rows, :] = d_top + contract_cols(d_pre, w_grid_up[...])

    def grad(k, *args, **kwargs):
        prog.poll()
        weight_grad(k, *args, **kwargs)
        prog.ready(k)

    stores[NCHUNK + 1].start()
    loaded(6, 13)
    grad(0, grid_lat, dpre_s, 512)
    grad(1, hid_s, dlin_s, 512)

    @tiles(2)
    def _(i, rows):
        out = tail_saved(1, contract_rows(mesh_t[:, rows], w_mesh_in[...]), rows, saves1)
        mesh_lat[rows, :] = out.astype(BF16)
        pick_src[rows, :] = pick(src_row[...].reshape(1, 768), i)
        pick_dst[rows, :] = pick(dst_row[...].reshape(1, 768), i)

    @tiles(3)
    def _(i, rows):
        out = tail_saved(2, contract_rows(edge_t[:, rows], w_edge_in[...]), rows, saves2)
        cat[rows, pl.ds(0, 512)] = out.astype(BF16)
        cat[rows, pl.ds(1024, 512)] = contract_rows(pick_dst[:, rows], mesh_lat[...]).astype(BF16)

    prog.poll()
    exchange(outgoing, incoming, 0, False)

    @pl.loop(0, 3)
    def _(i):
        rows = rows_of(i)
        cat[rows, pl.ds(512, 512)] = contract_rows(pick_src[:, rows], incoming[...]).astype(BF16)
        upd = tail_saved(3, matmul(cat[rows, :], w_edge_up[...]), rows, saves3)
        edge_new[rows, :] = (cat[rows, pl.ds(0, 512)].astype(F32) + upd).astype(BF16)

    @tiles(2)
    def _(i, rows):
        lat = mesh_lat[rows, :]
        agg_bf = matmul(pick_dst[rows, :], edge_new[...]).astype(BF16)
        agg[rows, :] = agg_bf
        pre = matmul(lat, w_mesh_up[pl.ds(0, 512), :]) + matmul(agg_bf, w_mesh_up[pl.ds(512, 512), :])
        upd, slope, normed, inv = tail(4, pre, rows, hid_s)
        mesh_out[rows, :] = (lat.astype(F32) + upd).astype(BF16)
        d_pre = tail_back(4, d_mesh_out[rows, :].astype(F32), slope, normed, inv, rows, dlin_s, dpre4)
        d_agg[rows, :] = contract_cols(d_pre, w_mesh_up[pl.ds(512, 512), :]).astype(BF16)

    @tiles(3)
    def _(i, rows):
        d_out = contract_rows(pick_dst[:, rows], d_agg[...])
        d_edge[rows, :] = d_out.astype(BF16)
        tail_back_saved(3, d_out, rows, saves3, dlin3, dpre3)

    @tiles(2)
    def _(i, rows):
        slot = matmul(pick_src[rows, :], dpre3[...]).astype(BF16)
        d_incoming[rows, :] = contract_cols(slot, w_edge_up[pl.ds(512, 512), :]).astype(BF16)

    exchange(d_incoming, d_outgoing, 1, True)
    stores[NCHUNK].start()
    grad(2, mesh_lat, dpre4, 512)
    grad(3, agg, dpre4, 512)
    grad(4, hid_s, dlin_s, 512)
    for part in range(3):
        grad(5 + part, cat, dpre3, 768, first=512 * part)
    grad(8, hid3, dlin3, 768)

    @tiles(3)
    def _(i, rows):
        d_out = d_edge[rows, :].astype(F32) + contract_cols(dpre3[rows, :], w_edge_up[pl.ds(0, 512), :])
        tail_back_saved(2, d_out, rows, saves2, dlin_s, dpre_s)

    misc[pl.ds(477, 4), :] = matmul(edge_t[...], dpre_s[...])
    grad(9, hid2, dlin_s, 768)

    @tiles(2)
    def _(i, rows):
        node = matmul(pick_dst[rows, :], dpre3[...]).astype(BF16)
        d_out = (d_mesh_out[rows, :].astype(F32) + contract_cols(dpre4[rows, :], w_mesh_up[pl.ds(0, 512), :])
                 + contract_cols(node, w_edge_up[pl.ds(1024, 512), :]))
        tail_back_saved(1, d_out, rows, saves1, dlin_s, dpre_s)

    misc[pl.ds(474, 3), :] = matmul(mesh_t[...], dpre_s[pl.ds(0, 512), :])
    grad(10, hid1, dlin_s, 512)
    prog.poll()
    exchange(d_incoming, d_outgoing, 1, False)

    @pl.loop(0, 2)
    def _(i):
        rows = rows_of(i)
        d_out = d_grid_lat[rows, :] + matmul(pick_send[rows, :], d_outgoing[...])
        d_pre = tail_back_saved(0, d_out, rows, saves0, dlin_s, dpre_s)
        d_grid_t[:, rows] = contract_cols(w_grid_in[...], d_pre)

    stores[NCHUNK + 2].start()
    grad(12, hid0, dlin_s, 512)
    prog.poll()
    misc[pl.ds(0, 474), :] = matmul(grid_t[...], dpre_s[pl.ds(0, 512), :])
    grads[11] = misc[...].astype(BF16)
    prog.ready(11)
    prog.poll()

    @pl.loop(0, NCHUNK)
    def _(k):
        red.drain(k)

    for copy in stores:
        copy.wait()


def fused_step(*args):
    def f32(*shape):
        return pltpu.VMEM(shape, F32)

    def bf16(*shape):
        return pltpu.VMEM(shape, BF16)

    def saves(n):
        return [bf16(n, 512), f32(n, 512), f32(n, 512), f32(n, 1)]

    scratch = [
        bf16(474, 512), bf16(474, 512), bf16(1536, 512), bf16(1024, 512), bf16(512, 512), bf16(6, 512, 512), bf16(512, 512),
        bf16(512, 512), bf16(512, 512), bf16(512, 512), f32(474, 512), bf16(NCHUNK, 512, 512),
        pltpu.SemaphoreType.DMA((13,)), pltpu.SemaphoreType.DMA((NCHUNK + 3,)),
        bf16(NCHUNK, 512, 512), bf16(NCHUNK, 256, 512), bf16(NCHUNK, 128, 512), bf16(NCHUNK, 64, 512), bf16(NCHUNK, 3, 64, 128),
        pltpu.SemaphoreType.DMA((NCHUNK, 12)), pltpu.SemaphoreType.DMA((NCHUNK, 12)),
        pltpu.SemaphoreType.DMA((2, 32)), pltpu.SemaphoreType.DMA((2, 32)),
        *saves(512), *saves(512), *saves(768), *saves(768),
        bf16(768, 512), bf16(768, 512), bf16(768, 512), bf16(768, 512), bf16(768, 512), bf16(512, 512),
        bf16(512, 512), bf16(512, 768), bf16(512, 768), bf16(512, 512), bf16(512, 512), bf16(768, 1536), bf16(768, 512),
        bf16(512, 512), bf16(512, 512), bf16(768, 512),
        bf16(512, 512), bf16(512, 512), bf16(512, 512), bf16(512, 512), f32(512, 512), bf16(8, 512), bf16(8, 512), f32(512, 512),
    ]
    return pl.pallas_call(
        step_kernel,
        out_shape=[jax.ShapeDtypeStruct((512, 512), BF16), jax.ShapeDtypeStruct((512, 512), BF16),
                   jax.ShapeDtypeStruct((474, 512), F32), jax.ShapeDtypeStruct((NCHUNK, 512, 512), BF16)],
        in_specs=[pl.BlockSpec(memory_space=pltpu.HBM if i in (0, 6, 9, 10, 11, 12, 14, 15) else pltpu.VMEM)
                  for i in range(len(args))],
        out_specs=[pl.BlockSpec(memory_space=pltpu.HBM)] * 4,
        scratch_shapes=scratch,
        compiler_params=pltpu.CompilerParams(collective_id=0, has_side_effects=True, vmem_limit_bytes=67043328),
    )(*args)


HOME = {0: (2, 0), 1: (3, 5), 2: (1, 0), 3: (1, 1), 4: (3, 4), 5: (0, 0), 6: (0, 1), 7: (0, 2), 8: (3, 3), 9: (3, 2), 10: (3, 1), 12: (3, 0)}


def spread_kernel(mesh_in, grid_in, d_grid_in, sums, mesh_out, grid_out, d_grid_out, edge_up, mesh_up, grid_up, second,
                  w_grid_h, w_mesh_h, w_edge_h, vecs_h, mesh_buf, grid_buf, d_grid_buf, sum_buf, wide, w_grid, w_mesh, w_edge, vecs,
                  sem_in, sem_out):
    loads = [pltpu.make_async_copy(sums.at[k], sum_buf.at[k], sem_in.at[k]) for k in range(NCHUNK)]
    through = [(mesh_in, mesh_buf, mesh_out), (grid_in, grid_buf, grid_out), (d_grid_in, d_grid_buf, d_grid_out)]
    heads = [pltpu.make_async_copy(a, b, sem_in.at[NCHUNK + i]) for i, (a, b, _) in enumerate(through)]
    tails = [pltpu.make_async_copy(b, c, sem_out.at[NCHUNK + i]) for i, (_, b, c) in enumerate(through)]
    loads[11].start()
    for k in range(NCHUNK):
        if k != 11:
            loads[k].start()
    for copy in heads:
        copy.start()
    outs = (edge_up, mesh_up, grid_up, second)
    stores = []
    loads[11].wait()
    misc = sum_buf[11].astype(F32)
    w_grid[...] = misc[:474]
    w_mesh[...] = misc[474:477]
    w_edge[...] = misc[477:481]
    for k in range(6):
        vecs[k] = misc[481 + 4 * k:485 + 4 * k]
    for i, (buf, out) in enumerate([(w_grid, w_grid_h), (w_mesh, w_mesh_h), (w_edge, w_edge_h), (vecs, vecs_h)]):
        stores.append(pltpu.make_async_copy(buf, out, sem_out.at[NCHUNK + 3 + i]))
        stores[-1].start()
    for k, (out, part) in HOME.items():
        loads[k].wait()

        @pl.loop(0, 8)
        def _(i):
            rows = rows_of(i, 64)
            wide[k, rows, :] = sum_buf[k, rows, :].astype(F32)

        home = outs[out].at[part] if out == 3 else outs[out].at[pl.ds(part * 512, 512)]
        stores.append(pltpu.make_async_copy(wide.at[k], home, sem_out.at[k]))
        stores[-1].start()
    for head, tail in zip(heads, tails):
        head.wait()
        tail.start()
    for copy in stores + tails:
        copy.wait()


def spread_out(*parts):
    def out(dtype, *shape):
        return jax.ShapeDtypeStruct(shape, dtype)

    anywhere = pl.BlockSpec(memory_space=pltpu.HBM)
    mesh_out, grid_out, d_grid, edge_up, mesh_up, grid_up, second, w_grid, w_mesh, w_edge, vecs = pl.pallas_call(
        spread_kernel,
        out_shape=[out(BF16, 512, 512), out(BF16, 512, 512), out(F32, 474, 512), out(F32, 1536, 512), out(F32, 1024, 512),
                   out(F32, 512, 512), out(F32, 6, 512, 512), out(F32, 474, 512), out(F32, 3, 512), out(F32, 4, 512),
                   out(F32, 6, 4, 512)],
        in_specs=[anywhere] * 4,
        out_specs=[anywhere] * 11,
        scratch_shapes=[pltpu.VMEM((512, 512), BF16), pltpu.VMEM((512, 512), BF16), pltpu.VMEM((474, 512), F32),
                        pltpu.VMEM((NCHUNK, 512, 512), BF16), pltpu.VMEM((NCHUNK, 512, 512), F32),
                        pltpu.VMEM((474, 512), F32), pltpu.VMEM((3, 512), F32), pltpu.VMEM((4, 512), F32),
                        pltpu.VMEM((6, 4, 512), F32),
                        pltpu.SemaphoreType.DMA((NCHUNK + 3,)), pltpu.SemaphoreType.DMA((NCHUNK + 7,))],
        compiler_params=pltpu.CompilerParams(vmem_limit_bytes=67043328),
    )(*parts)
    return mesh_out, grid_out, d_grid, w_grid, w_mesh, w_edge, edge_up, mesh_up, grid_up, second, vecs


def solution(mesh):
    row_spec = P(AXIS_NAME, None)
    edge_spec = P(AXIS_NAME)
    rep_spec = P()
    in_specs = (row_spec, row_spec, row_spec, row_spec, edge_spec, edge_spec) + (rep_spec,) * 8 + (row_spec, row_spec)
    out_specs = (row_spec, row_spec, row_spec) + (rep_spec,) * 8

    def local_step(grid_in, mesh_static, edge_static, send_rows, edge_src, edge_dst, *rest):
        parts = fused_step(grid_in.T, mesh_static.T, edge_static.T, send_rows.T,
                           edge_src, edge_dst, *rest)
        mesh_out, grid_out, d_grid_t, *sums = spread_out(*parts)
        return (mesh_out, grid_out, d_grid_t.T) + tuple(sums)

    return jax.shard_map(local_step, mesh=mesh, in_specs=in_specs, out_specs=out_specs, check_vma=False)
```

```python
import jax
import jax.numpy as jnp
from jax import lax
from jax.experimental import pallas as pl
from jax.experimental.pallas import tpu as pltpu
from jax.sharding import PartitionSpec as P

LN_EPS = 1e-5
AXIS_NAME = 'gp'
NCHUNK = 13
TILE = 256
LATENT = 512
F32 = jnp.float32
BF16 = jnp.bfloat16


def matmul(lhs, rhs):
    return jnp.dot(lhs, rhs, preferred_element_type=jnp.float32)


def contract_rows(lhs, rhs):
    return lax.dot_general(lhs, rhs, (((0,), (0,)), ((), ())), preferred_element_type=jnp.float32)


def contract_cols(lhs, rhs):
    return lax.dot_general(lhs, rhs, (((1,), (1,)), ((), ())), preferred_element_type=jnp.float32)


class Place:
    def __init__(self):
        self.p = lax.axis_index(AXIS_NAME)
        self.c = self.p % 2
        self.x = (self.p // 2) % 2
        self.y = (self.p // 4) % 2
        self.z = self.p // 8
        self.core_peer = self.p + 1 - 2 * self.c
        self.x_peer = self.p + 2 - 4 * self.x
        self.y_peer = self.p + 4 - 8 * self.y

    def z_peer(self, j):
        return self.p % 8 + ((self.z + 1 + j) % 4) * 8


class Reducer:
    def __init__(self, at, grads, out, r0, r1, r2, r3, send, recv):
        self.at = at
        self.grads, self.out = grads, out
        self.r0, self.r1, self.r2, self.r3 = r0, r1, r2, r3
        self.send, self.recv = send, recv

    def spot(self, k):
        at = self.at
        odd = k % 2
        d1 = at.x * (1 - odd) + at.y * odd
        d2 = at.y * (1 - odd) + at.x * odd
        p1 = at.x_peer * (1 - odd) + at.y_peer * odd
        p2 = at.y_peer * (1 - odd) + at.x_peer * odd
        return d1, d2, p1, p2

    def copies(self, s, k):
        at = self.at
        d1, d2, p1, p2 = self.spot(k)

        def make(src, dst, lane, dev):
            return pltpu.make_async_remote_copy(
                src_ref=src, dst_ref=dst, send_sem=self.send.at[k, lane], recv_sem=self.recv.at[k, lane],
                device_id=(dev,), device_id_type=pl.DeviceIdType.MESH)

        def rows(start, size):
            return pl.ds(pl.multiple_of(start, 64), size)

        row1 = at.c * 256 + d1 * 128
        row2 = row1 + d2 * 64
        if s == 0:
            return [make(self.grads.at[k, rows((1 - at.c) * 256, 256)], self.r0.at[k], 0, at.core_peer)]
        if s == 1:
            return [make(self.grads.at[k, rows(at.c * 256 + (1 - d1) * 128, 128)], self.r1.at[k], 1, p1)]
        if s == 2:
            return [make(self.grads.at[k, rows(row1 + (1 - d2) * 64, 64)], self.r2.at[k], 2, p2)]
        if s == 3:
            cols = [pl.ds(pl.multiple_of(((at.z + 1 + j) % 4) * 128, 128), 128) for j in range(3)]
            return [make(self.grads.at[k, rows(row2, 64), cols[j]], self.r3.at[k, j], 3 + j, at.z_peer(j)) for j in range(3)]
        if s == 4:
            part = self.out.at[k, rows(row2, 64), pl.ds(pl.multiple_of(at.z * 128, 128), 128)]
            return [make(part, part, 6 + j, at.z_peer(j)) for j in range(3)]
        if s == 5:
            part = self.out.at[k, rows(row2, 64)]
            return [make(part, part, 9, p2)]
        if s == 6:
            part = self.out.at[k, rows(row1, 128)]
            return [make(part, part, 10, p1)]
        part = self.out.at[k, rows(at.c * 256, 256)]
        return [make(part, part, 11, at.core_peer)]

    def start(self, s, k):
        for copy in self.copies(s, k):
            copy.start()

    def stage(self, s, k):
        at = self.at
        d1, d2, _, _ = self.spot(k)
        for copy in self.copies(s, k):
            copy.wait_recv()
        row1 = at.c * 256 + d1 * 128
        row2 = row1 + d2 * 64
        if s < 3:
            start, size, landed = ((at.c * 256, 256, self.r0), (row1, 128, self.r1), (row2, 64, self.r2))[s]

            @pl.loop(0, size // 64)
            def _(i):
                mine = (k, pl.ds(pl.multiple_of(start + i * 64, 64), 64))
                theirs = landed[k, pl.ds(pl.multiple_of(i * 64, 64), 64)]
                self.grads[mine] = (self.grads[mine].astype(F32) + theirs.astype(F32)).astype(BF16)
        elif s == 3:
            spot = (k, pl.ds(pl.multiple_of(row2, 64), 64), pl.ds(pl.multiple_of(at.z * 128, 128), 128))
            total = self.grads[spot].astype(F32)
            for j in range(3):
                total = total + self.r3[k, j].astype(F32)
            self.out[spot] = total.astype(BF16)
        if s < 7:
            self.start(s + 1, k)

    def drain(self, k):
        for s in range(8):
            for copy in self.copies(s, k):
                copy.wait_send()


ORDER = (
        (),
        (),
        (),
        (),
        (0, 1),
        (16, 17),
        (32,),
        (),
        (),
        (),
        (),
        (),
        (),
        (),
        (33,),
        (2,),
        (48, 3),
        (4, 5),
        (19, 6, 18),
        (8, 20),
        (49, 34, 7, 21),
        (64, 35),
        (22, 9, 65, 36, 10),
        (37, 23, 80, 50, 24, 81, 12, 38, 51, 11, 25, 52, 26, 39, 53, 97, 40, 66, 96, 68, 67, 54, 27, 55, 41, 42, 112,
     69, 28, 113, 82, 70, 83, 56, 43, 44, 85, 84, 57, 71, 98, 58, 100, 86, 72, 59, 87, 99, 114, 60, 101, 73, 74, 88,
     116, 115, 102, 75, 89, 76, 90, 117, 103, 104, 91, 105, 92, 119, 106, 121, 120, 107, 118, 108, 122, 123, 124),
)


class Progress:
    def __init__(self, red, stores):
        self.red, self.stores, self.point = red, stores, 0

    def ready(self, k):
        self.red.start(0, k)

    def poll(self):
        for code in ORDER[self.point]:
            self.red.stage(code // 16, code % 16)
            if code // 16 == 7:
                self.stores[code % 16].start()
        self.point += 1


def rows_of(i, tile=TILE):
    return pl.ds(pl.multiple_of(i * tile, tile), tile)


def step_kernel(grid_h, mesh_t, edge_t, send_t, src_row, dst_row, w_grid_in_h, w_mesh_in, w_edge_in, w_edge_up_h,
                w_mesh_up_h, w_grid_up_h, w_second_h, vectors, d_mesh_out_h, d_grid_out_h,
                mesh_out_h, grid_out_h, d_grid_h, sums_h,
                grid_t, w_grid_in, w_edge_up, w_mesh_up, w_grid_up, w_second, d_mesh_out, d_grid_out,
                mesh_out, grid_out, d_grid_t, sums, load_sem, store_sem,
                grads, r0, r1, r2, r3, red_send, red_recv, a2a_send, a2a_recv,
                hid0, dsl0, nrm0, inv0, hid1, dsl1, nrm1, inv1, hid2, dsl2, nrm2, inv2, hid3, dsl3, nrm3, inv3,
                hid_s, dlin_s, dpre_s, dlin3, dpre3, dpre4,
                pick_send, pick_src, pick_dst, grid_lat, mesh_lat, cat, edge_new, agg, d_agg, d_edge,
                outgoing, incoming, d_incoming, d_outgoing, d_grid_lat, d_node, d_slot, misc):
    at = Place()
    n_dev = 32
    moves = [(grid_h, grid_t), (w_grid_in_h, w_grid_in), (w_second_h.at[0], w_second.at[0]), (w_grid_up_h, w_grid_up),
             (w_second_h.at[5], w_second.at[5]), (d_grid_out_h, d_grid_out), (w_second_h.at[1], w_second.at[1]),
             (w_second_h.at[2], w_second.at[2]), (w_edge_up_h, w_edge_up), (w_second_h.at[3], w_second.at[3]),
             (w_mesh_up_h, w_mesh_up), (w_second_h.at[4], w_second.at[4]), (d_mesh_out_h, d_mesh_out)]
    loads = [pltpu.make_async_copy(src, dst, load_sem.at[i]) for i, (src, dst) in enumerate(moves)]
    for copy in loads:
        copy.start()
    stores = [pltpu.make_async_copy(sums.at[k], sums_h.at[k], store_sem.at[k]) for k in range(NCHUNK)]
    stores += [pltpu.make_async_copy(src, dst, store_sem.at[NCHUNK + i]) for i, (src, dst) in enumerate(
        [(mesh_out, mesh_out_h), (grid_out, grid_out_h), (d_grid_t, d_grid_h)])]

    def loaded(first, last):
        for copy in loads[first:last]:
            copy.wait()

    barrier = pltpu.get_barrier_semaphore()

    @pl.loop(1, n_dev)
    def _(r):
        pl.semaphore_signal(barrier, inc=1, device_id=((at.p + r) % n_dev,), device_id_type=pl.DeviceIdType.MESH)

    red = Reducer(at, grads, sums, r0, r1, r2, r3, red_send, red_recv)
    prog = Progress(red, stores)

    def vec(k, j):
        return vectors[k, pl.ds(j, 1), :]

    def tail(k, pre, rows, hid):
        pre = pre + vec(k, 0)
        sig = jax.nn.sigmoid(pre)
        act = pre * sig
        hid_bf = act.astype(BF16)
        hid[rows, :] = hid_bf
        out_lin = matmul(hid_bf, w_second[k]) + vec(k, 1)
        centered = out_lin - jnp.mean(out_lin, axis=-1, keepdims=True)
        inv = lax.rsqrt(jnp.mean(centered * centered, axis=-1, keepdims=True) + LN_EPS)
        normed = centered * inv
        return normed * vec(k, 2) + vec(k, 3), sig + act * (1.0 - sig), normed, inv

    def tail_saved(k, pre, rows, saves):
        hid, dsl, nrm, inv_ref = saves
        out, slope, normed, inv = tail(k, pre, rows, hid)
        dsl[rows, :] = slope
        nrm[rows, :] = normed
        inv_ref[rows, :] = inv
        return out

    def tail_back(k, d_out, slope, normed, inv, rows, dlin, dpre):
        d_normed = d_out * vec(k, 2)
        d_lin = inv * (d_normed - jnp.mean(d_normed, axis=-1, keepdims=True)
                       - normed * jnp.mean(d_normed * normed, axis=-1, keepdims=True))
        d_lin_bf = d_lin.astype(BF16)
        dlin[rows, :] = d_lin_bf
        d_pre = contract_cols(d_lin_bf, w_second[k]) * slope
        d_pre_bf = d_pre.astype(BF16)
        dpre[rows, :] = d_pre_bf
        for j, term in enumerate((d_pre, d_lin, d_out * normed, d_out)):
            spot = pl.ds(481 + 4 * k + j, 1)
            misc[spot, :] = misc[spot, :] + jnp.sum(term, axis=0, keepdims=True)
        return d_pre_bf

    def tail_back_saved(k, d_out, rows, saves, dlin, dpre):
        _, dsl, nrm, inv_ref = saves
        return tail_back(k, d_out, dsl[rows, :], nrm[rows, :], inv_ref[rows, :], rows, dlin, dpre)

    def weight_grad(k, lhs, rhs, n_rows, first=0):
        @pl.loop(0, LATENT // TILE)
        def _(i):
            cols = pl.ds(pl.multiple_of(first + i * TILE, TILE), TILE)
            part = contract_rows(lhs[pl.ds(0, n_rows), cols], rhs[pl.ds(0, n_rows), :])
            grads[k, rows_of(i), :] = part.astype(BF16)

    def exchange(src, dst, lane, start):
        def copy(r):
            to = (at.p + r) % n_dev
            return pltpu.make_async_remote_copy(
                src_ref=src.at[pl.ds(pl.multiple_of(to * 16, 16), 16)], dst_ref=dst.at[pl.ds(pl.multiple_of(at.p * 16, 16), 16)],
                send_sem=a2a_send.at[lane, r], recv_sem=a2a_recv.at[lane, r],
                device_id=(to,), device_id_type=pl.DeviceIdType.MESH)

        if start:
            @pl.loop(1, n_dev)
            def _(r):
                copy(r).start()

            mine = pl.ds(pl.multiple_of(at.p * 16, 16), 16)
            dst[mine, :] = src[mine, :]
        else:
            @pl.loop(1, n_dev)
            def _(r):
                copy(r).wait()

    saves0 = (hid0, dsl0, nrm0, inv0)
    saves1 = (hid1, dsl1, nrm1, inv1)
    saves2 = (hid2, dsl2, nrm2, inv2)
    saves3 = (hid3, dsl3, nrm3, inv3)
    misc[pl.ds(472, 40), :] = jnp.zeros((40, LATENT), F32)

    def tiles(n):
        def run(body):
            prog.poll()

            @pl.loop(0, n)
            def _(i):
                body(i, rows_of(i))
        return run

    slots = send_t[...]
    spread = jnp.where(lax.broadcasted_iota(jnp.int32, (32, 512), 0) == lax.broadcasted_iota(jnp.int32, (32, 512), 1) // 16,
                       1.0, 0.0).astype(BF16)
    slots = (matmul((slots // 32).astype(F32).astype(BF16), spread) * 32.0
             + matmul((slots % 32).astype(F32).astype(BF16), spread))
    own = lax.broadcasted_iota(jnp.int32, (16, 512), 0) == lax.broadcasted_iota(jnp.int32, (16, 512), 1) % 16
    send_row = jnp.sum(jnp.where(own, slots, 0.0), axis=0, keepdims=True)

    def pick(row, i):
        ids = lax.broadcasted_iota(jnp.int32, (TILE, row.shape[1]), 0) + i * TILE
        return jnp.where(ids == row, 1.0, 0.0).astype(BF16)

    send_ids = send_row.astype(jnp.int32)
    for i in range(2):
        pick_send[rows_of(i), :] = pick(send_ids, i)

    loaded(0, 3)

    @pl.loop(0, 2)
    def _(i):
        rows = rows_of(i)
        out = tail_saved(0, contract_rows(grid_t[:, rows], w_grid_in[...]), rows, saves0)
        grid_lat[rows, :] = out.astype(BF16)

    @pl.loop(0, 2)
    def _(i):
        rows = rows_of(i)
        outgoing[rows, :] = contract_rows(pick_send[:, rows], grid_lat[...]).astype(BF16)

    pl.semaphore_wait(barrier, n_dev - 1)
    exchange(outgoing, incoming, 0, True)
    loaded(3, 6)

    @tiles(2)
    def _(i, rows):
        lat = grid_lat[rows, :]
        upd, slope, normed, inv = tail(5, matmul(lat, w_grid_up[...]), rows, hid_s)
        grid_out[rows, :] = (lat.astype(F32) + upd).astype(BF16)
        d_top = d_grid_out[rows, :].astype(F32)
        d_pre = tail_back(5, d_top, slope, normed, inv, rows, dlin_s, dpre_s)
        d_grid_lat[rows, :] = d_top + contract_cols(d_pre, w_grid_up[...])

    def grad(k, *args, **kwargs):
        prog.poll()
        weight_grad(k, *args, **kwargs)
        prog.ready(k)

    stores[NCHUNK + 1].start()
    loaded(6, 13)
    grad(0, grid_lat, dpre_s, 512)
    grad(1, hid_s, dlin_s, 512)

    @tiles(2)
    def _(i, rows):
        out = tail_saved(1, contract_rows(mesh_t[:, rows], w_mesh_in[...]), rows, saves1)
        mesh_lat[rows, :] = out.astype(BF16)
        pick_src[rows, :] = pick(src_row[...].reshape(1, 768), i)
        pick_dst[rows, :] = pick(dst_row[...].reshape(1, 768), i)

    @tiles(3)
    def _(i, rows):
        out = tail_saved(2, contract_rows(edge_t[:, rows], w_edge_in[...]), rows, saves2)
        cat[rows, pl.ds(0, 512)] = out.astype(BF16)
        cat[rows, pl.ds(1024, 512)] = contract_rows(pick_dst[:, rows], mesh_lat[...]).astype(BF16)

    prog.poll()
    exchange(outgoing, incoming, 0, False)

    @pl.loop(0, 3)
    def _(i):
        rows = rows_of(i)
        cat[rows, pl.ds(512, 512)] = contract_rows(pick_src[:, rows], incoming[...]).astype(BF16)
        upd = tail_saved(3, matmul(cat[rows, :], w_edge_up[...]), rows, saves3)
        edge_new[rows, :] = (cat[rows, pl.ds(0, 512)].astype(F32) + upd).astype(BF16)

    @tiles(2)
    def _(i, rows):
        lat = mesh_lat[rows, :]
        agg_bf = matmul(pick_dst[rows, :], edge_new[...]).astype(BF16)
        agg[rows, :] = agg_bf
        pre = matmul(lat, w_mesh_up[pl.ds(0, 512), :]) + matmul(agg_bf, w_mesh_up[pl.ds(512, 512), :])
        upd, slope, normed, inv = tail(4, pre, rows, hid_s)
        mesh_out[rows, :] = (lat.astype(F32) + upd).astype(BF16)
        d_pre = tail_back(4, d_mesh_out[rows, :].astype(F32), slope, normed, inv, rows, dlin_s, dpre4)
        d_agg[rows, :] = contract_cols(d_pre, w_mesh_up[pl.ds(512, 512), :]).astype(BF16)

    @tiles(3)
    def _(i, rows):
        d_out = contract_rows(pick_dst[:, rows], d_agg[...])
        d_edge[rows, :] = d_out.astype(BF16)
        tail_back_saved(3, d_out, rows, saves3, dlin3, dpre3)

    @tiles(2)
    def _(i, rows):
        slot = matmul(pick_src[rows, :], dpre3[...]).astype(BF16)
        d_incoming[rows, :] = contract_cols(slot, w_edge_up[pl.ds(512, 512), :]).astype(BF16)

    exchange(d_incoming, d_outgoing, 1, True)
    stores[NCHUNK].start()
    grad(2, mesh_lat, dpre4, 512)
    grad(3, agg, dpre4, 512)
    grad(4, hid_s, dlin_s, 512)
    for part in range(3):
        grad(5 + part, cat, dpre3, 768, first=512 * part)
    grad(8, hid3, dlin3, 768)

    @tiles(3)
    def _(i, rows):
        d_out = d_edge[rows, :].astype(F32) + contract_cols(dpre3[rows, :], w_edge_up[pl.ds(0, 512), :])
        tail_back_saved(2, d_out, rows, saves2, dlin_s, dpre_s)

    misc[pl.ds(477, 4), :] = matmul(edge_t[...], dpre_s[...])
    grad(9, hid2, dlin_s, 768)

    @tiles(2)
    def _(i, rows):
        node = matmul(pick_dst[rows, :], dpre3[...]).astype(BF16)
        d_out = (d_mesh_out[rows, :].astype(F32) + contract_cols(dpre4[rows, :], w_mesh_up[pl.ds(0, 512), :])
                 + contract_cols(node, w_edge_up[pl.ds(1024, 512), :]))
        tail_back_saved(1, d_out, rows, saves1, dlin_s, dpre_s)

    misc[pl.ds(474, 3), :] = matmul(mesh_t[...], dpre_s[pl.ds(0, 512), :])
    grad(10, hid1, dlin_s, 512)
    prog.poll()
    exchange(d_incoming, d_outgoing, 1, False)

    @pl.loop(0, 2)
    def _(i):
        rows = rows_of(i)
        d_out = d_grid_lat[rows, :] + matmul(pick_send[rows, :], d_outgoing[...])
        d_pre = tail_back_saved(0, d_out, rows, saves0, dlin_s, dpre_s)
        d_grid_t[:, rows] = contract_cols(w_grid_in[...], d_pre)

    stores[NCHUNK + 2].start()
    grad(12, hid0, dlin_s, 512)
    prog.poll()
    misc[pl.ds(0, 474), :] = matmul(grid_t[...], dpre_s[pl.ds(0, 512), :])
    grads[11] = misc[...].astype(BF16)
    prog.ready(11)
    prog.poll()

    @pl.loop(0, NCHUNK)
    def _(k):
        red.drain(k)

    for copy in stores:
        copy.wait()


def fused_step(*args):
    def f32(*shape):
        return pltpu.VMEM(shape, F32)

    def bf16(*shape):
        return pltpu.VMEM(shape, BF16)

    def saves(n):
        return [bf16(n, 512), f32(n, 512), f32(n, 512), f32(n, 1)]

    scratch = [
        bf16(474, 512), bf16(474, 512), bf16(1536, 512), bf16(1024, 512), bf16(512, 512), bf16(6, 512, 512), bf16(512, 512),
        bf16(512, 512), bf16(512, 512), bf16(512, 512), f32(474, 512), bf16(NCHUNK, 512, 512),
        pltpu.SemaphoreType.DMA((13,)), pltpu.SemaphoreType.DMA((NCHUNK + 3,)),
        bf16(NCHUNK, 512, 512), bf16(NCHUNK, 256, 512), bf16(NCHUNK, 128, 512), bf16(NCHUNK, 64, 512), bf16(NCHUNK, 3, 64, 128),
        pltpu.SemaphoreType.DMA((NCHUNK, 12)), pltpu.SemaphoreType.DMA((NCHUNK, 12)),
        pltpu.SemaphoreType.DMA((2, 32)), pltpu.SemaphoreType.DMA((2, 32)),
        *saves(512), *saves(512), *saves(768), *saves(768),
        bf16(768, 512), bf16(768, 512), bf16(768, 512), bf16(768, 512), bf16(768, 512), bf16(512, 512),
        bf16(512, 512), bf16(512, 768), bf16(512, 768), bf16(512, 512), bf16(512, 512), bf16(768, 1536), bf16(768, 512),
        bf16(512, 512), bf16(512, 512), bf16(768, 512),
        bf16(512, 512), bf16(512, 512), bf16(512, 512), bf16(512, 512), f32(512, 512), bf16(8, 512), bf16(8, 512), f32(512, 512),
    ]
    return pl.pallas_call(
        step_kernel,
        out_shape=[jax.ShapeDtypeStruct((512, 512), BF16), jax.ShapeDtypeStruct((512, 512), BF16),
                   jax.ShapeDtypeStruct((474, 512), F32), jax.ShapeDtypeStruct((NCHUNK, 512, 512), BF16)],
        in_specs=[pl.BlockSpec(memory_space=pltpu.HBM if i in (0, 6, 9, 10, 11, 12, 14, 15) else pltpu.VMEM)
                  for i in range(len(args))],
        out_specs=[pl.BlockSpec(memory_space=pltpu.HBM)] * 4,
        scratch_shapes=scratch,
        compiler_params=pltpu.CompilerParams(collective_id=0, has_side_effects=True, vmem_limit_bytes=67043328),
    )(*args)


HOME = {0: (2, 0), 1: (3, 5), 2: (1, 0), 3: (1, 1), 4: (3, 4), 5: (0, 0), 6: (0, 1), 7: (0, 2), 8: (3, 3), 9: (3, 2), 10: (3, 1), 12: (3, 0)}


def spread_kernel(mesh_in, grid_in, d_grid_in, sums, mesh_out, grid_out, d_grid_out, edge_up, mesh_up, grid_up, second,
                  w_grid_h, w_mesh_h, w_edge_h, vecs_h, mesh_buf, grid_buf, d_grid_buf, sum_buf, wide, w_grid, w_mesh, w_edge, vecs,
                  sem_in, sem_out):
    loads = [pltpu.make_async_copy(sums.at[k], sum_buf.at[k], sem_in.at[k]) for k in range(NCHUNK)]
    through = [(mesh_in, mesh_buf, mesh_out), (grid_in, grid_buf, grid_out), (d_grid_in, d_grid_buf, d_grid_out)]
    heads = [pltpu.make_async_copy(a, b, sem_in.at[NCHUNK + i]) for i, (a, b, _) in enumerate(through)]
    tails = [pltpu.make_async_copy(b, c, sem_out.at[NCHUNK + i]) for i, (_, b, c) in enumerate(through)]
    loads[11].start()
    for k in range(NCHUNK):
        if k != 11:
            loads[k].start()
    for copy in heads:
        copy.start()
    outs = (edge_up, mesh_up, grid_up, second)
    stores = []
    loads[11].wait()
    misc = sum_buf[11].astype(F32)
    w_grid[...] = misc[:474]
    w_mesh[...] = misc[474:477]
    w_edge[...] = misc[477:481]
    for k in range(6):
        vecs[k] = misc[481 + 4 * k:485 + 4 * k]
    for i, (buf, out) in enumerate([(w_grid, w_grid_h), (w_mesh, w_mesh_h), (w_edge, w_edge_h), (vecs, vecs_h)]):
        stores.append(pltpu.make_async_copy(buf, out, sem_out.at[NCHUNK + 3 + i]))
        stores[-1].start()
    for k, (out, part) in HOME.items():
        loads[k].wait()

        @pl.loop(0, 8)
        def _(i):
            rows = rows_of(i, 64)
            wide[k, rows, :] = sum_buf[k, rows, :].astype(F32)

        home = outs[out].at[part] if out == 3 else outs[out].at[pl.ds(part * 512, 512)]
        stores.append(pltpu.make_async_copy(wide.at[k], home, sem_out.at[k]))
        stores[-1].start()
    for head, tail in zip(heads, tails):
        head.wait()
        tail.start()
    for copy in stores + tails:
        copy.wait()


def spread_out(*parts):
    def out(dtype, *shape):
        return jax.ShapeDtypeStruct(shape, dtype)

    anywhere = pl.BlockSpec(memory_space=pltpu.HBM)
    mesh_out, grid_out, d_grid, edge_up, mesh_up, grid_up, second, w_grid, w_mesh, w_edge, vecs = pl.pallas_call(
        spread_kernel,
        out_shape=[out(BF16, 512, 512), out(BF16, 512, 512), out(F32, 474, 512), out(F32, 1536, 512), out(F32, 1024, 512),
                   out(F32, 512, 512), out(F32, 6, 512, 512), out(F32, 474, 512), out(F32, 3, 512), out(F32, 4, 512),
                   out(F32, 6, 4, 512)],
        in_specs=[anywhere] * 4,
        out_specs=[anywhere] * 11,
        scratch_shapes=[pltpu.VMEM((512, 512), BF16), pltpu.VMEM((512, 512), BF16), pltpu.VMEM((474, 512), F32),
                        pltpu.VMEM((NCHUNK, 512, 512), BF16), pltpu.VMEM((NCHUNK, 512, 512), F32),
                        pltpu.VMEM((474, 512), F32), pltpu.VMEM((3, 512), F32), pltpu.VMEM((4, 512), F32),
                        pltpu.VMEM((6, 4, 512), F32),
                        pltpu.SemaphoreType.DMA((NCHUNK + 3,)), pltpu.SemaphoreType.DMA((NCHUNK + 7,))],
        compiler_params=pltpu.CompilerParams(vmem_limit_bytes=67043328),
    )(*parts)
    return mesh_out, grid_out, d_grid, w_grid, w_mesh, w_edge, edge_up, mesh_up, grid_up, second, vecs


def solution(mesh):
    row_spec = P(AXIS_NAME, None)
    edge_spec = P(AXIS_NAME)
    rep_spec = P()
    in_specs = (row_spec, row_spec, row_spec, row_spec, edge_spec, edge_spec) + (rep_spec,) * 8 + (row_spec, row_spec)
    out_specs = (row_spec, row_spec, row_spec) + (rep_spec,) * 8

    def local_step(grid_in, mesh_static, edge_static, send_rows, edge_src, edge_dst, *rest):
        parts = fused_step(grid_in.T, mesh_static.T, edge_static.T, send_rows.T,
                           edge_src, edge_dst, *rest)
        mesh_out, grid_out, d_grid_t, *sums = spread_out(*parts)
        return (mesh_out, grid_out, d_grid_t.T) + tuple(sums)

    return jax.shard_map(local_step, mesh=mesh, in_specs=in_specs, out_specs=out_specs, check_vma=False)
```
